32 devices in a mesh: dp: 8 (over z, x), hyper: 4 (over y, core).
Axes of the slice: x: 2, y: 2, z: 4, core: 2. Of those that a mesh axis runs over, the one named last changes fastest.
Arguments:
- inputs: bfloat16 [64, 64, 128], P(('dp', 'hyper')), may hold values from -64 to 64
- labels: int32 [64, 64], P(('dp', 'hyper')), may hold values from 0 to 255
- client_ids: int32 [64], P(('dp', 'hyper')), may hold values from 0 to 63
- ext_weight: bfloat16 [128, 4096], replicated, may hold values from -0.5 to 0.5
- ext_bias: bfloat16 [4096], replicated, may hold values from -3 to 3
- embeddings: bfloat16 [64, 128], replicated, may hold values from -1.5 to 1.5
- hyper_in: bfloat16 [128, 50], replicated, may hold values from -2.09375 to 2.09375
- hyper_bias: float32 [50], replicated, may hold values from -3 to 3
- hyper_out: bfloat16 [4096, 50, 256], P('hyper'), may hold values from -0.1796875 to 0.1796875
Outputs:
- grad_ext_weight: float32 [128, 4096], replicated
- grad_ext_bias: float32 [4096], replicated
- grad_embeddings: float32 [64, 128], replicated
- grad_hyper_in: float32 [128, 50], replicated
- grad_hyper_bias: float32 [50], replicated
- grad_hyper_out: float32 [4096, 50, 256], P(('hyper', 'dp'))
The draws below stay inside these ranges and needn't reach their ends.
Inputs may be any that keep to these rules, and one draw needn't show every extreme that they name: `client_ids`: A client may hold several slots or none.
All inputs are finite; a program needn't handle non-finite values.
Results may differ from the reference program's by a relative error of at most 0.014.
The reference program's roundings to bfloat16 on the way count: a program that leaves them out, or rounds other values in their place, can miss the bound.
Values may be sent and summed in bfloat16 or wider, within the bound.
A program may use at most 192 MiB of HBM per device.

```python
import jax
import jax.numpy as jnp
from jax import lax

D = 4096
C = 256
DIN = 128
HH = 50
E = 128
CD = 2
R = 64
SLOTS = 64
NCL = 64
N_DP = 8
N_HYPER = 4


def draw_inputs(key, part):
    values = jax.random.normal(key, (SLOTS, R, DIN), jnp.float32)
    values = jnp.clip(values, -6.0, 6.0)
    return jnp.clip(values, -64.0, 64.0).astype(jnp.bfloat16)


def with_ends(result, key, low, high):
    shape = result.shape
    place = [jax.random.randint(jax.random.fold_in(key, axis), (), 0, shape[axis]) for axis in range(len(shape))]
    result = result.at[tuple(place)].set(low)
    longest = shape.index(max(shape))
    place[longest] = (place[longest] + 1) % shape[longest]
    return result.at[tuple(place)].set(high)


def block_scale(rng, dims, cuts, smallest, high):
    loudness = 1.0
    for axis_at, shards_of in cuts:
        draws = jax.random.uniform(jax.random.fold_in(jax.random.fold_in(rng, 6), axis_at), (shards_of,), jnp.float32, smallest / len(cuts), high / len(cuts))
        loudness = loudness * jnp.repeat(jnp.exp(draws), dims[axis_at] // shards_of).reshape((-1,) + (1,) * (len(dims) - 1 - axis_at))
    return loudness


def gaussian(own_key, extent, spread, bound, shards=(), kind=jnp.bfloat16):
    loudness = block_scale(own_key, extent, shards, -0.22, 0.18) if shards else 1.0
    array = jax.random.normal(own_key, extent, jnp.float32) * spread * loudness
    return jnp.minimum(jnp.maximum(array, -bound), bound).astype(kind)


def setup_inputs(seed: int = 0) -> dict:
    splits = jax.random.split(jax.random.key(seed), 10)
    return {
        "inputs": draw_inputs(jax.random.fold_in(splits[9], 71), 0),
        "labels": with_ends(jax.random.randint(splits[1], (SLOTS, R), 0, C), jax.random.fold_in(splits[1], 1), 0, C - 1).astype(jnp.int32),
        "client_ids": with_ends(jax.random.randint(splits[2], (SLOTS,), 0, NCL), jax.random.fold_in(splits[2], 1), 0, NCL - 1).astype(jnp.int32),
        "ext_weight": gaussian(splits[3], (DIN, D), DIN ** -0.5, 0.5),
        "ext_bias": gaussian(splits[4], (D,), 0.5, 3.0),
        "embeddings": gaussian(splits[5], (NCL, E), 0.25, 1.5),
        "hyper_in": gaussian(splits[6], (E, HH), 0.35, 2.09375),
        "hyper_bias": gaussian(splits[7], (HH,), 0.5, 3.0, (), jnp.float32),
        "hyper_out": gaussian(splits[8], (D, HH, C), 0.03, 0.1796875, ((0, 4),)),
    }


highest = lax.Precision.HIGHEST


def silu_slope(values):
    logistic = jax.nn.sigmoid(values)
    return logistic * (1.0 + values * (1.0 - logistic))


def class_grads(logits, slot_labels, row_count):
    largest = jnp.max(logits, axis=-1, keepdims=True)
    exponent = jnp.exp(logits - largest)
    probability = exponent / jnp.sum(exponent, axis=-1, keepdims=True)
    classes = jnp.arange(logits.shape[-1], dtype=jnp.int32)
    onehot = (slot_labels[..., None] == classes).astype(jnp.float32)
    return ((probability - onehot) / row_count).astype(jnp.bfloat16)


def reference(inputs, labels, client_ids, ext_weight, ext_bias, embeddings, hyper_in, hyper_bias, hyper_out):
    group_size = N_HYPER * CD
    hyper_wide = hyper_out.astype(jnp.float32)
    hyper_in_wide = hyper_in.astype(jnp.float32)
    client_table = jnp.arange(NCL, dtype=jnp.int32)

    def one_group(totals, group_index):
        first_slot = (group_index * group_size).astype(jnp.int32)
        slot_inputs = lax.dynamic_slice_in_dim(inputs, first_slot, group_size, 0)
        slot_labels = lax.dynamic_slice_in_dim(labels, first_slot, group_size, 0)
        slot_ids = lax.dynamic_slice_in_dim(client_ids, first_slot, group_size, 0)
        flat_in = slot_inputs.reshape(group_size * R, DIN)
        preact = jnp.dot(flat_in, ext_weight, preferred_element_type=jnp.float32) + ext_bias.astype(jnp.float32)
        features = jax.nn.silu(preact).astype(jnp.bfloat16).reshape(group_size, R, D)
        picked = embeddings[slot_ids]
        hyper_preact = jnp.dot(picked, hyper_in, preferred_element_type=jnp.float32) + hyper_bias
        hidden = jax.nn.silu(hyper_preact).astype(jnp.bfloat16)
        client_heads = jnp.einsum("kh,dhc->kdc", hidden.astype(jnp.float32), hyper_wide).astype(jnp.bfloat16)
        feat_wide = features.astype(jnp.float32)
        heads_wide = client_heads.astype(jnp.float32)
        logits = jnp.einsum("krd,kdc->krc", feat_wide, heads_wide)
        dlogits = class_grads(logits, slot_labels, R)
        dlog_wide = dlogits.astype(jnp.float32)
        dheads = jnp.einsum("krd,krc->kdc", feat_wide, dlog_wide).astype(jnp.bfloat16)
        dfeatures = jnp.einsum("krc,kdc->krd", dlog_wide, heads_wide).astype(jnp.bfloat16)
        dpreact = (dfeatures.reshape(group_size * R, D).astype(jnp.float32) * silu_slope(preact)).astype(jnp.bfloat16)
        grad_weight = jnp.dot(flat_in.T, dpreact, preferred_element_type=jnp.float32)
        grad_bias = jnp.sum(dpreact.astype(jnp.float32), axis=0)
        dheads_wide = dheads.astype(jnp.float32)
        group_out = jnp.einsum("kh,kdc->dhc", hidden.astype(jnp.float32), dheads_wide)
        group_out = lax.optimization_barrier(group_out.astype(jnp.bfloat16)).astype(jnp.float32)
        dhidden = jnp.einsum("kdc,dhc->kh", dheads_wide, hyper_wide)
        hyper_dpre = dhidden * silu_slope(hyper_preact)
        grad_in = jnp.dot(picked.astype(jnp.float32).T, hyper_dpre, precision=highest)
        grad_hbias = jnp.sum(hyper_dpre, axis=0)
        select = (slot_ids[:, None] == client_table[None, :]).astype(jnp.float32)
        grad_table = jnp.dot(select.T, jnp.dot(hyper_dpre, hyper_in_wide.T, precision=highest), precision=highest)
        updated = (totals[0] + grad_weight, totals[1] + grad_bias, totals[2] + grad_table,
                   totals[3] + grad_in, totals[4] + grad_hbias, totals[5] + group_out)
        return updated, None

    initial = (jnp.zeros((DIN, D), jnp.float32), jnp.zeros((D,), jnp.float32), jnp.zeros((NCL, E), jnp.float32),
               jnp.zeros((E, HH), jnp.float32), jnp.zeros((HH,), jnp.float32), jnp.zeros((D, HH, C), jnp.float32))
    totals, unused = lax.scan(one_group, initial, jnp.arange(N_DP, dtype=jnp.int32))
    return (totals[0], totals[1], totals[2], totals[3], totals[4], totals[5])
```

```python
import functools

import jax
import jax.numpy as jnp
from jax import lax
from jax.experimental import pallas as pl
from jax.experimental.pallas import tpu as pltpu
from jax.sharding import PartitionSpec as P

highest = lax.Precision.HIGHEST
f32 = jnp.float32
bf16 = jnp.bfloat16
i32 = jnp.int32
VM = pl.BlockSpec(memory_space=pltpu.VMEM)
DG = 16
LIMIT = 60 * 1024 * 1024


def silu_slope(values):
    logistic = jax.nn.sigmoid(values)
    return logistic * (1.0 + values * (1.0 - logistic))


def dot(a, b, dims=((1,), (0,)), **kw):
    return lax.dot_general(a, b, (dims, ((), ())), preferred_element_type=f32, **kw)


def swap(index, other, count):
    if count & (count - 1):
        return lax.rem(index + other, count)
    out = index
    bit = 1
    while bit < count:
        if other & bit:
            out = out + bit - 2 * bit * lax.rem(index // bit, 2)
        bit *= 2
    return out


def source(index, other, count):
    if count & (count - 1):
        return lax.rem(index + count - other, count)
    return swap(index, other, count)


def place():
    i, j = lax.axis_index("dp"), lax.axis_index("hyper")
    return i, j, j + 1 - 2 * lax.rem(j, 2)


def barrier(i, j, n_dp, hyper_peers):
    sem = pltpu.get_barrier_semaphore()
    for t in range(1, n_dp):
        pl.semaphore_signal(sem, 1, device_id={"dp": swap(i, t, n_dp), "hyper": j})
    for peer in hyper_peers:
        pl.semaphore_signal(sem, 1, device_id={"dp": i, "hyper": peer})
    pl.semaphore_wait(sem, n_dp - 1 + len(hyper_peers))


def remote(src, dst, send, recv, dp, hyper):
    return pltpu.make_async_remote_copy(
        src_ref=src, dst_ref=dst, send_sem=send, recv_sem=recv, device_id={"dp": dp, "hyper": hyper}
    )


def gather_blocks(own, out, i, j, partner, n_dp, half, s1, r1, s2, r2, s3, r3):
    n_hyper = 2 * half
    sends = []

    def start(copy):
        copy.start()
        sends.append(copy)
        return copy

    first = {}
    for t in range(1, n_dp):
        first[t] = start(remote(own, out.at[i, j], s1.at[t], r1.at[t], swap(i, t, n_dp), j))
    second, third = {}, {}
    for t in range(n_dp):
        at = source(i, t, n_dp)
        if t:
            first[t].wait_recv()
        block = out.at[at, j] if t else own
        for u in range(1, half):
            second[t, u] = start(
                remote(block, out.at[at, j], s2.at[t, u], r2.at[t, u], i, lax.rem(j + 2 * u, n_hyper))
            )
        third[t, 0] = start(remote(block, out.at[at, j], s3.at[t, 0], r3.at[t, 0], i, partner))
    for t in range(n_dp):
        at = source(i, t, n_dp)
        for u in range(1, half):
            second[t, u].wait_recv()
            peer = lax.rem(j + n_hyper - 2 * u, n_hyper)
            third[t, u] = start(
                remote(out.at[at, peer], out.at[at, peer], s3.at[t, u], r3.at[t, u], i, partner)
            )
    for copy in third.values():
        copy.wait_recv()
    for copy in sends:
        copy.wait_send()


def gather_sems(n_dp, half):
    dma = pltpu.SemaphoreType.DMA
    return [dma((n_dp,)), dma((n_dp,))] + [dma((n_dp, half)) for _ in range(4)]


def same_parity(j, half):
    return [lax.rem(j + 2 * u, 2 * half) for u in range(1, half)]


def gather_kernel(n_dp, half, x_ref, out_ref, *sems):
    i, j, partner = place()
    barrier(i, j, n_dp, same_parity(j, half) + [partner])
    out_ref[i, j] = x_ref[...]
    gather_blocks(x_ref, out_ref, i, j, partner, n_dp, half, *sems)


def comm_params(number):
    return pltpu.CompilerParams(collective_id=number, has_side_effects=True, vmem_limit_bytes=LIMIT)


def gather_all(x, n_dp, n_hyper):
    return pl.pallas_call(
        functools.partial(gather_kernel, n_dp, n_hyper // 2),
        out_shape=jax.ShapeDtypeStruct((n_dp, n_hyper) + x.shape, x.dtype),
        in_specs=[VM],
        out_specs=VM,
        scratch_shapes=gather_sems(n_dp, n_hyper // 2),
        compiler_params=comm_params(0),
        name="gather_inputs",
    )(x)


def spread(hidden, kinds):
    k, h = hidden.shape
    rows = lax.broadcasted_iota(i32, (k * DG, k), 0) // DG
    pick = (rows == lax.broadcasted_iota(i32, (k * DG, k), 1)).astype(bf16)
    tall = dot(pick, hidden).astype(bf16)
    columns = lax.broadcasted_iota(i32, (h, h * DG), 1) // DG
    widen = (columns == lax.broadcasted_iota(i32, (h, h * DG), 0)).astype(bf16)
    full = dot(tall, widen)
    d = lax.broadcasted_iota(i32, full.shape, 0) % DG
    same = d == lax.broadcasted_iota(i32, full.shape, 1) % DG
    return jnp.where(same, full, 0.0).astype(bf16)


def spread_t(hidden):
    k, h = hidden.shape
    rows = lax.broadcasted_iota(i32, (h * DG, h), 0) // DG
    pick = (rows == lax.broadcasted_iota(i32, (h * DG, h), 1)).astype(bf16)
    tall = dot(pick, hidden, ((1,), (1,))).astype(bf16)
    columns = lax.broadcasted_iota(i32, (k, k * DG), 1) // DG
    widen = (columns == lax.broadcasted_iota(i32, (k, k * DG), 0)).astype(bf16)
    full = dot(tall, widen)
    d = lax.broadcasted_iota(i32, full.shape, 0) % DG
    same = d == lax.broadcasted_iota(i32, full.shape, 1) % DG
    return jnp.where(same, full, 0.0).astype(bf16)


def forward_kernel(own, rows, where_ref, x_ref, hid_ref, w_ref, b_ref, ho_ref, part_ref, diag, heads):
    step = pl.program_id(0)
    blocks = x_ref.shape[1]
    group = blocks * own
    wide = w_ref.shape[1]
    classes = ho_ref.shape[2]
    hh = ho_ref.shape[0]

    @pl.when(step == 0)
    def _():
        diag[...] = spread(hid_ref[...], None)
        part_ref[...] = jnp.zeros_like(part_ref)

    for g in range(wide // DG):
        rhs = ho_ref[:, g * DG : (g + 1) * DG, :].reshape(hh * DG, classes)
        out = dot(diag[...], rhs).astype(bf16)
        heads[:, g * DG : (g + 1) * DG, :] = out.reshape(group, DG, classes)
    for p in range(blocks):
        pre = dot(x_ref[0, p, : own * rows, :], w_ref[...]) + b_ref[...]
        feat = (pre / (1.0 + jnp.exp(-pre))).astype(bf16)
        for s in range(own):
            part_ref[p, s * rows : (s + 1) * rows, :] += dot(
                feat[s * rows : (s + 1) * rows], heads[p * own + s]
            )


def forward(where, gathered, hidden, ext_weight, ext_bias, ho, own, rows):
    n_dp, n_hyper, tall, width = gathered.shape
    hh, wide, classes = ho.shape
    chunk = 128
    group = own * n_hyper
    steps = wide // chunk
    return pl.pallas_call(
        functools.partial(forward_kernel, own, rows),
        out_shape=jax.ShapeDtypeStruct((n_hyper, own * rows, classes), f32),
        grid_spec=pltpu.PrefetchScalarGridSpec(
            num_scalar_prefetch=1,
            grid=(steps,),
            in_specs=[
                pl.BlockSpec((1, n_hyper, tall, width), lambda s, at: (at[0], 0, 0, 0)),
                pl.BlockSpec((group, hh), lambda s, at: (0, 0)),
                pl.BlockSpec((width, chunk), lambda s, at: (0, at[1] * steps + s)),
                pl.BlockSpec((1, chunk), lambda s, at: (0, at[1] * steps + s)),
                pl.BlockSpec((hh, chunk, classes), lambda s, at: (0, s, 0)),
            ],
            out_specs=pl.BlockSpec((n_hyper, own * rows, classes), lambda s, at: (0, 0, 0)),
            scratch_shapes=[
                pltpu.VMEM((group * DG, hh * DG), bf16),
                pltpu.VMEM((group, chunk, classes), bf16),
            ],
        ),
        compiler_params=pltpu.CompilerParams(vmem_limit_bytes=LIMIT),
        name="forward_part",
    )(where, gathered, hidden, ext_weight, ext_bias, ho)


def logits_kernel(n_dp, half, part, labels, out_ref, from_partner, summed, from_peer, own_dl, sp, rp, sq, rq, *sems):
    i, j, partner = place()
    n_hyper = 2 * half
    barrier(i, j, n_dp, same_parity(j, half) + [partner])
    to_partner = {}
    for u in list(range(1, half)) + [0]:
        to_partner[u] = remote(
            part.at[lax.rem(partner + 2 * u, n_hyper)], from_partner.at[u], sp.at[u], rp.at[u], i, partner
        )
        to_partner[u].start()
    to_peer = {}
    for u in range(1, half):
        peer = lax.rem(j + 2 * u, n_hyper)
        to_partner[u].wait_recv()
        summed[u] = part[peer] + from_partner[u]
        to_peer[u] = remote(summed.at[u], from_peer.at[u], sq.at[u], rq.at[u], i, peer)
        to_peer[u].start()
    to_partner[0].wait_recv()
    logits = part[j] + from_partner[0]
    for u in range(1, half):
        to_peer[u].wait_recv()
        logits = logits + from_peer[u]
    largest = jnp.max(logits, axis=-1, keepdims=True)
    exponent = jnp.exp(logits - largest)
    probability = exponent / jnp.sum(exponent, axis=-1, keepdims=True)
    onehot = (labels[...] == lax.broadcasted_iota(i32, logits.shape, 1)).astype(f32)
    dl = ((probability - onehot) / ROWS[0]).astype(bf16)
    own_dl[...] = dl
    out_ref[i, j] = dl
    gather_blocks(own_dl, out_ref, i, j, partner, n_dp, half, *sems)
    for copy in list(to_partner.values()) + list(to_peer.values()):
        copy.wait_send()


ROWS = [64]


def logits_and_gather(part, labels, n_dp, n_hyper, rows):
    half = n_hyper // 2
    _, tall, classes = part.shape
    dma = pltpu.SemaphoreType.DMA
    ROWS[0] = rows
    return pl.pallas_call(
        functools.partial(logits_kernel, n_dp, half),
        out_shape=jax.ShapeDtypeStruct((n_dp, n_hyper, tall, classes), bf16),
        in_specs=[VM, VM],
        out_specs=VM,
        scratch_shapes=[
            pltpu.VMEM((half, tall, classes), f32),
            pltpu.VMEM((half, tall, classes), f32),
            pltpu.VMEM((half, tall, classes), f32),
            pltpu.VMEM((tall, classes), bf16),
        ]
        + [dma((half,)) for _ in range(4)]
        + gather_sems(n_dp, half),
        compiler_params=comm_params(1),
        name="logits_exchange",
    )(part, labels)


def backward_kernel(own, rows, where_ref, dl_ref, x_ref, hid_ref, w_ref, b_ref, ho_ref,
                    gw_ref, gb_ref, go_ref, dh_ref, diag, diag_t, heads, dheads, feats, slopes, dpre, total):
    step = pl.program_id(0)
    dpc, n_hyper = dl_ref.shape[:2]
    hh, narrow, classes = ho_ref.shape
    width = x_ref.shape[3]
    groups = narrow // DG
    slots = dpc * n_hyper * own
    tall = own * rows
    hidden = hid_ref[...]
    diag[...] = spread(hidden, None)
    diag_t[...] = spread_t(hidden)

    @pl.when(step == 0)
    def _():
        gw_ref[...] = jnp.zeros_like(gw_ref)
        gb_ref[...] = jnp.zeros_like(gb_ref)
        go_ref[...] = jnp.zeros_like(go_ref)

    def ho_group(g):
        return ho_ref[:, pl.ds(pl.multiple_of(g * DG, DG), DG), :].reshape(hh * DG, classes)

    def heads_step(g, carry):
        out = dot(diag[...], ho_group(g)).astype(bf16)
        heads[:, pl.ds(pl.multiple_of(g * DG, DG), DG), :] = out.reshape(slots, DG, classes)
        return carry

    lax.fori_loop(0, groups, heads_step, 0)

    def features_step(a, carry):
        for p in range(n_hyper):
            pre = dot(x_ref[a, p, :tall, :], w_ref[...]) + b_ref[...]
            logistic = 1.0 / (1.0 + jnp.exp(-pre))
            at = pl.ds(pl.multiple_of((a * n_hyper + p) * tall, tall), tall)
            feats[at, :] = (pre * logistic).astype(bf16)
            slopes[at, :] = logistic * (1.0 + pre * (1.0 - logistic))
        return carry

    lax.fori_loop(0, dpc, features_step, 0)

    def slots_step(a, carry):
        for p in range(n_hyper):
            for s in range(own):
                block = a * n_hyper + p
                slot = block * own + s
                dl = dl_ref[a, p, s * rows : (s + 1) * rows, :]
                at = pl.ds(pl.multiple_of(block * tall + s * rows, rows), rows)
                dhead = dot(feats[at, :], dl, ((0,), (0,))).astype(bf16)
                dheads[:, pl.ds(pl.multiple_of(slot * DG, DG), DG), :] = dhead.reshape(groups, DG, classes)
                dfeat = dot(dl, heads[slot], ((1,), (1,))).astype(bf16)
                dpre[at, :] = (dfeat.astype(f32) * slopes[at, :]).astype(bf16)
        return carry

    lax.fori_loop(0, dpc, slots_step, 0)

    def weight_step(a, carry):
        gw, gb = carry
        for p in range(n_hyper):
            at = pl.ds(pl.multiple_of((a * n_hyper + p) * tall, tall), tall)
            block = dpre[at, :]
            gw = gw + dot(x_ref[a, p, :tall, :], block, ((0,), (0,)))
            gb = gb + jnp.sum(block.astype(f32), axis=0, keepdims=True)
        return gw, gb

    zero = (jnp.zeros((width, narrow), f32), jnp.zeros((1, narrow), f32))
    gw, gb = lax.fori_loop(0, dpc, weight_step, zero)
    gw_ref[...] += gw
    gb_ref[...] += gb
    total[...] = jnp.zeros_like(total)

    def out_step(g, carry):
        block = dheads[g]
        at = pl.ds(pl.multiple_of(g * DG, DG), DG)
        go_ref[:, at, :] += dot(diag_t[...], block).reshape(hh, DG, classes)
        total[...] += dot(block, ho_group(g), ((1,), (1,)))
        return carry

    lax.fori_loop(0, groups, out_step, 0)
    d = lax.broadcasted_iota(i32, total.shape, 0) % DG
    same = d == lax.broadcasted_iota(i32, total.shape, 1) % DG
    kept = jnp.where(same, total[...], 0.0).reshape(slots, DG, hh * DG)
    kept = jnp.sum(kept, axis=1)
    columns = lax.broadcasted_iota(i32, (hh * DG, hh), 0) // DG
    fold = (columns == lax.broadcasted_iota(i32, (hh * DG, hh), 1)).astype(f32)
    dh_ref[...] = dot(kept, fold, precision=highest)


def backward(where, dl_all, gathered, hidden, w, b, ho, own, rows):
    n_dp, n_hyper, tall, width = gathered.shape
    hh, wide, classes = ho.shape
    narrow = wide // n_dp
    group = own * n_hyper
    dpc = max(1, 64 // group)
    slots = dpc * group
    samples = slots * rows
    return pl.pallas_call(
        functools.partial(backward_kernel, own, rows),
        out_shape=(
            jax.ShapeDtypeStruct((width, narrow), f32),
            jax.ShapeDtypeStruct((1, narrow), f32),
            jax.ShapeDtypeStruct((hh, narrow, classes), f32),
            jax.ShapeDtypeStruct((n_dp * group, hh), f32),
        ),
        grid_spec=pltpu.PrefetchScalarGridSpec(
            num_scalar_prefetch=1,
            grid=(n_dp // dpc,),
            in_specs=[
                pl.BlockSpec((dpc, n_hyper, own * rows, classes), lambda s, at: (s, 0, 0, 0)),
                pl.BlockSpec((dpc, n_hyper, tall, width), lambda s, at: (s, 0, 0, 0)),
                pl.BlockSpec((slots, hh), lambda s, at: (s, 0)),
                pl.BlockSpec((width, narrow), lambda s, at: (0, 0)),
                pl.BlockSpec((1, narrow), lambda s, at: (0, 0)),
                pl.BlockSpec((hh, narrow, classes), lambda s, at: (0, at[0], 0)),
            ],
            out_specs=[
                pl.BlockSpec((width, narrow), lambda s, at: (0, 0)),
                pl.BlockSpec((1, narrow), lambda s, at: (0, 0)),
                pl.BlockSpec((hh, narrow, classes), lambda s, at: (0, 0, 0)),
                pl.BlockSpec((slots, hh), lambda s, at: (s, 0)),
            ],
            scratch_shapes=[
                pltpu.VMEM((slots * DG, hh * DG), bf16),
                pltpu.VMEM((hh * DG, slots * DG), bf16),
                pltpu.VMEM((slots, narrow, classes), bf16),
                pltpu.VMEM((narrow // DG, slots * DG, classes), bf16),
                pltpu.VMEM((samples, narrow), bf16),
                pltpu.VMEM((samples, narrow), f32),
                pltpu.VMEM((samples, narrow), bf16),
                pltpu.VMEM((slots * DG, hh * DG), f32),
            ],
        ),
        compiler_params=pltpu.CompilerParams(vmem_limit_bytes=LIMIT),
        name="backward_part",
    )(where, dl_all, gathered, hidden, w, b, ho)


def final_kernel(n_dp, half, x_ref, dh_ref, out_ref, tot_ref, b1, b2, mine, sa, ra, sb, rb, sc, rc, *sems):
    i, j, partner = place()
    n_hyper = 2 * half
    peers = [lax.rem(j + u, n_hyper) for u in range(1, n_hyper)]
    barrier(i, j, n_dp, peers)
    sends = []
    to_hyper = []
    for u in range(1, n_hyper):
        copy = remote(dh_ref.at[peers[u - 1]], b1.at[u], sa.at[u], ra.at[u], i, peers[u - 1])
        copy.start()
        to_hyper.append(copy)
    out_ref[i, j] = x_ref[...]
    quarter = dh_ref[j]
    for u in range(1, n_hyper):
        to_hyper[u - 1].wait_recv()
        quarter = quarter + b1[u]
    mine[0] = quarter
    b2[i] = quarter
    to_dp = []
    for t in range(1, n_dp):
        copy = remote(mine.at[0], b2.at[i], sb.at[t], rb.at[t], swap(i, t, n_dp), j)
        copy.start()
        to_dp.append(copy)
    gather_blocks(x_ref, out_ref, i, j, partner, n_dp, half, *sems)
    for copy in to_dp:
        copy.wait_recv()
    total = b2[0]
    for t in range(1, n_dp):
        total = total + b2[t]
    mine[1] = total
    tot_ref[j] = total
    last = []
    for u in range(1, n_hyper):
        copy = remote(mine.at[1], tot_ref.at[j], sc.at[u], rc.at[u], i, peers[u - 1])
        copy.start()
        last.append(copy)
    for copy in last:
        copy.wait_recv()
    for copy in to_hyper + to_dp + last:
        copy.wait_send()


def final_exchange(x, dh, n_dp, n_hyper):
    dma = pltpu.SemaphoreType.DMA
    part = dh.shape[1:]
    return pl.pallas_call(
        functools.partial(final_kernel, n_dp, n_hyper // 2),
        out_shape=(
            jax.ShapeDtypeStruct((n_dp, n_hyper) + x.shape, x.dtype),
            jax.ShapeDtypeStruct(dh.shape, f32),
        ),
        in_specs=[VM, VM],
        out_specs=(VM, VM),
        scratch_shapes=[
            pltpu.VMEM((n_hyper,) + part, f32),
            pltpu.VMEM((n_dp,) + part, f32),
            pltpu.VMEM((2,) + part, f32),
            dma((n_hyper,)), dma((n_hyper,)), dma((n_dp,)), dma((n_dp,)), dma((n_hyper,)), dma((n_hyper,)),
        ]
        + gather_sems(n_dp, n_hyper // 2),
        compiler_params=comm_params(2),
        name="final_exchange",
    )(x, dh)


def local(
    inputs, labels, client_ids, ext_weight, ext_bias, embeddings, hyper_in, hyper_bias, hyper_out
):
    n_dp, n_hyper = lax.axis_size("dp"), lax.axis_size("hyper")
    i, j = lax.axis_index("dp"), lax.axis_index("hyper")
    own, rows, width_in = inputs.shape
    wide, hh, classes = hyper_out.shape
    narrow = wide // n_dp
    group = own * n_hyper
    slots = group * n_dp
    tall = own * rows

    parts_of_ids = jnp.stack([client_ids // 256, client_ids % 256]).astype(bf16)
    flat_own = inputs.reshape(tall, width_in)
    packed = jnp.concatenate([flat_own, jnp.pad(parts_of_ids, ((0, 14), (0, width_in - own)))])
    gathered = gather_all(packed, n_dp, n_hyper)
    table = jnp.arange(embeddings.shape[0], dtype=i32)
    halves = gathered[:, :, tall : tall + 2, :own].astype(f32).astype(i32)
    ids = (halves[:, :, 0] * 256 + halves[:, :, 1]).reshape(-1)
    select = ids[:, None] == table[None, :]
    picked = jnp.dot(select.astype(bf16), embeddings, preferred_element_type=f32).astype(bf16)
    hyper_preact = jnp.dot(picked, hyper_in, preferred_element_type=f32) + hyper_bias
    hidden = jax.nn.silu(hyper_preact).astype(bf16)

    where = jnp.stack([i, j]).astype(i32)
    ho = hyper_out.transpose(1, 0, 2)
    wide_bias = ext_bias.astype(f32)[None]
    hidden_group = lax.dynamic_slice_in_dim(hidden, i * group, group, 0)
    part = forward(where, gathered, hidden_group, ext_weight, wide_bias, ho, own, rows)
    dl_all = logits_and_gather(part, labels.reshape(tall, 1), n_dp, n_hyper, rows)

    start = (j * n_dp + i) * narrow
    w = lax.dynamic_slice_in_dim(ext_weight, start, narrow, 1)
    b = lax.dynamic_slice_in_dim(wide_bias, start, narrow, 1)
    gw, gb, grad_out, dh = backward(where, dl_all, gathered, hidden, w, b, ho, own, rows)
    sent = jnp.concatenate([gw, jnp.pad(gb, ((0, 15), (0, 0)))]).astype(bf16)
    dh = jnp.pad(dh, ((0, 0), (0, 128 - hh))).reshape(n_hyper, slots // n_hyper, 128)
    gw_all, dhidden = final_exchange(sent, dh, n_dp, n_hyper)
    dhidden = dhidden.reshape(slots, 128)[:, :hh]
    hyper_dpre = dhidden * silu_slope(hyper_preact)
    grad_in = jnp.dot(picked.astype(f32).T, hyper_dpre, precision=highest)
    grad_hbias = jnp.sum(hyper_dpre, axis=0)
    back_rows = jnp.dot(hyper_dpre, hyper_in.astype(f32).T, precision=highest)
    grad_table = jnp.dot(select.astype(f32).T, back_rows, precision=highest)
    grad_weight = gw_all[:, :, :width_in].transpose(2, 1, 0, 3).reshape(width_in, -1).astype(f32)
    grad_bias = gw_all[:, :, width_in].transpose(1, 0, 2).reshape(-1).astype(f32)
    return (grad_weight, grad_bias, grad_table, grad_in, grad_hbias, grad_out.transpose(1, 0, 2))


def solution(mesh):
    placed = (
        P(("dp", "hyper"), None, None),
        P(("dp", "hyper"), None),
        P(("dp", "hyper")),
        P(),
        P(),
        P(),
        P(),
        P(),
        P("hyper", None, None),
    )
    return jax.shard_map(
        local,
        mesh=mesh,
        in_specs=placed,
        out_specs=(P(), P(), P(), P(), P(), P(("hyper", "dp"), None, None)),
        check_vma=False,
    )
```

```python
import functools

import jax
import jax.numpy as jnp
from jax import lax
from jax.experimental import pallas as pl
from jax.experimental.pallas import tpu as pltpu
from jax.sharding import PartitionSpec as P

highest = lax.Precision.HIGHEST
f32 = jnp.float32
bf16 = jnp.bfloat16
i32 = jnp.int32
VM = pl.BlockSpec(memory_space=pltpu.VMEM)
DG = 16
LIMIT = 60 * 1024 * 1024


def silu_slope(values):
    logistic = jax.nn.sigmoid(values)
    return logistic * (1.0 + values * (1.0 - logistic))


def dot(a, b, dims=((1,), (0,)), **kw):
    return lax.dot_general(a, b, (dims, ((), ())), preferred_element_type=f32, **kw)


def swap(index, other, count):
    if count & (count - 1):
        return lax.rem(index + other, count)
    out = index
    bit = 1
    while bit < count:
        if other & bit:
            out = out + bit - 2 * bit * lax.rem(index // bit, 2)
        bit *= 2
    return out


def source(index, other, count):
    if count & (count - 1):
        return lax.rem(index + count - other, count)
    return swap(index, other, count)


def place():
    i, j = lax.axis_index("dp"), lax.axis_index("hyper")
    return i, j, j + 1 - 2 * lax.rem(j, 2)


def spread(hidden):
    k, h = hidden.shape
    rows = lax.broadcasted_iota(i32, (k * DG, k), 0) // DG
    pick = (rows == lax.broadcasted_iota(i32, (k * DG, k), 1)).astype(bf16)
    tall = dot(pick, hidden).astype(bf16)
    columns = lax.broadcasted_iota(i32, (h, h * DG), 1) // DG
    widen = (columns == lax.broadcasted_iota(i32, (h, h * DG), 0)).astype(bf16)
    full = dot(tall, widen)
    d = lax.broadcasted_iota(i32, full.shape, 0) % DG
    same = d == lax.broadcasted_iota(i32, full.shape, 1) % DG
    return jnp.where(same, full, 0.0).astype(bf16)


def spread_t(hidden):
    k, h = hidden.shape
    rows = lax.broadcasted_iota(i32, (h * DG, h), 0) // DG
    pick = (rows == lax.broadcasted_iota(i32, (h * DG, h), 1)).astype(bf16)
    tall = dot(pick, hidden, ((1,), (1,))).astype(bf16)
    columns = lax.broadcasted_iota(i32, (k, k * DG), 1) // DG
    widen = (columns == lax.broadcasted_iota(i32, (k, k * DG), 0)).astype(bf16)
    full = dot(tall, widen)
    d = lax.broadcasted_iota(i32, full.shape, 0) % DG
    same = d == lax.broadcasted_iota(i32, full.shape, 1) % DG
    return jnp.where(same, full, 0.0).astype(bf16)


def remote(src, dst, send, recv, dp, hyper):
    return pltpu.make_async_remote_copy(
        src_ref=src, dst_ref=dst, send_sem=send, recv_sem=recv, device_id={"dp": dp, "hyper": hyper}
    )


class Flood:
    def __init__(self, out, sems, n_dp, half):
        self.out, self.sems = out, sems
        self.na, self.half, self.n_hyper = n_dp // 2, half, 2 * half
        self.i, self.j, self.partner = place()
        self.a, self.b = self.i // 2, lax.rem(self.i, 2)
        self.cut = out.shape[2] // 32 * 16
        self.tall = out.shape[2]
        self.copies = {}

    @staticmethod
    def scratch(n_dp, half):
        dma, na = pltpu.SemaphoreType.DMA, n_dp // 2
        shapes = [(na,), (na,), (na, half), (na, half), (na, half), (na, 2, half)]
        return [dma(s) for s in shapes for _ in range(2)]

    def at(self, t, b, u):
        dp = source(self.a, t, self.na) * 2 + (self.b if b == 0 else 1 - self.b)
        return dp, lax.rem(self.j + self.n_hyper - 2 * u, self.n_hyper)

    def send(self, kind, index, block, where, dp, hyper, rows=None):
        number = "zxypqc".index(kind)
        s, r = self.sems[2 * number], self.sems[2 * number + 1]
        target = self.out.at[where[0], where[1]]
        if rows is not None:
            block, target = block.at[pl.ds(*rows)], target.at[pl.ds(*rows)]
        copy = remote(block, target, s.at[index], r.at[index], dp, hyper)
        copy.start()
        self.copies[kind, index] = copy

    def recv(self, kind, index):
        self.copies[kind, index].wait_recv()

    def peers(self):
        return [(u, lax.rem(self.j + 2 * u, self.n_hyper)) for u in range(1, self.half)]

    def column(self, t, own=None):
        where = self.at(t, 0, 0)
        if t:
            self.recv("z", (t,))
        block = self.out.at[where[0], where[1]] if own is None else own
        for u, peer in self.peers():
            self.send("y", (t, u), block, where, self.i, peer)
        self.send("x", (t,), block, where, self.a * 2 + 1 - self.b, self.j)
        self.send("c", (t, 0, 0), block, where, self.i, self.partner)

    def begin(self, own):
        where = self.at(0, 0, 0)
        for t in range(1, self.na):
            self.send("z", (t,), own, where, swap(self.a, t, self.na) * 2 + self.b, self.j)
        self.column(0, own)

    def pair(self, t):
        where = self.at(t, 1, 0)
        self.recv("x", (t,))
        block = self.out.at[where[0], where[1]]
        for u, peer in self.peers():
            self.send("p", (t, u), block, where, self.i, peer, (0, self.cut))
        self.send("c", (t, 1, 0), block, where, self.i, self.partner)

    def across(self, t):
        for u, peer in self.peers():
            where = self.at(t, 0, u)
            self.recv("y", (t, u))
            block = self.out.at[where[0], where[1]]
            self.send("c", (t, 0, u), block, where, self.i, self.partner)
            self.send(
                "q", (t, u), block, where, self.a * 2 + 1 - self.b, self.j, (self.cut, self.tall - self.cut)
            )

    def corner(self, t):
        for u, peer in self.peers():
            where = self.at(t, 1, u)
            self.recv("p", (t, u))
            self.recv("q", (t, u))
            self.send("c", (t, 1, u), self.out.at[where[0], where[1]], where, self.i, self.partner)

    def near(self, t):
        for u in range(self.half):
            self.recv("c", (t, 0, u))

    def far(self, t):
        for u in range(self.half):
            self.recv("c", (t, 1, u))

    def end(self):
        for copy in self.copies.values():
            copy.wait_send()


def hypernet(tiles, own, emb, hin_t, hb):
    blocks = tiles.shape[0]
    tiles = tiles.astype(f32)
    ids = (tiles[:, :8] * 256.0 + tiles[:, 8:]).reshape(blocks * 8, tiles.shape[2])[:, :1]
    clients = emb.shape[0]
    wide = (ids == lax.broadcasted_iota(i32, (blocks * 8, clients), 1).astype(f32)).astype(f32).astype(bf16)
    slots = blocks * own
    row = lax.broadcasted_iota(i32, (slots, blocks * 8), 0)
    column = lax.broadcasted_iota(i32, (slots, blocks * 8), 1)
    keep = (column == row // own * 8 + row % own).astype(f32).astype(bf16)
    select = dot(keep, wide).astype(bf16)
    picked = dot(select, emb).astype(bf16)
    preact = dot(picked, hin_t, ((1,), (1,))) + hb
    hidden = (preact / (1.0 + jnp.exp(-preact))).astype(bf16)
    return select, picked, preact, hidden


def main_kernel(
    n_dp, half, own, rows, aligned,
    x_ref, ids_ref, lab_ref, ew_ref, eb_ref, wn_ref, bn_ref, emb_ref, hin_ref, hb_ref, ho_ref,
    gw_all, dh_all, dheads_out, hid_out, pre_out, picked_out, select_out,
    packed, xg, dl_all, own_dl, w_wide, w_narrow, bufs, ho_n, diag_f, heads_f, part,
    from_partner, summed, from_peer, diag, heads, dheads, feats, slopes, dpre, total,
    gw_acc, gb_acc, gw_own, dh_mine, b1, b2, dh_sum, local_sems, buf_sems,
    sp, rp, sq, rq, sa, ra, sb, rb, sc, rc, *floods
):
    count = len(floods) // 3
    i, j, partner = place()
    n_hyper = 2 * half
    tall, width = x_ref.shape
    hh, wide, classes = ho_ref.shape
    chunk = bufs.shape[2]
    chunks = wide // chunk
    narrow = wide // n_dp
    groups = narrow // DG
    depth = bufs.shape[0]
    slots = n_dp * n_hyper * own
    group = n_hyper * own
    CS = diag.shape[0] // DG

    def buffer(c, slot):
        at = pl.ds(pl.multiple_of(c * chunk, chunk), chunk)
        return pltpu.make_async_copy(ho_ref.at[:, at, :], bufs.at[slot], buf_sems.at[slot])

    for c in range(min(depth, chunks)):
        buffer(c, c).start()
    wide_at = pl.ds(pl.multiple_of(j * wide, 128), wide)
    get_w = pltpu.make_async_copy(ew_ref.at[:, wide_at], w_wide, local_sems.at[0])
    get_w.start()
    get_h = pltpu.make_async_copy(
        ho_ref.at[:, pl.ds(pl.multiple_of(i * narrow, narrow), narrow), :], ho_n, local_sems.at[1]
    )
    get_h.start()
    first = (j * n_dp + i) * narrow
    if aligned:
        narrow_at = pl.ds(pl.multiple_of(first, 128), narrow)
        get_n = pltpu.make_async_copy(ew_ref.at[:, narrow_at], w_narrow, local_sems.at[2])
        get_n.start()

    row = lax.broadcasted_iota(i32, (16, width), 0)
    tile = jnp.zeros((16, width), f32)
    for s in range(own):
        number = ids_ref[s]
        tile = jnp.where(row == s, (number // 256).astype(f32), tile)
        tile = jnp.where(row == 8 + s, (number % 256).astype(f32), tile)
    packed[:tall] = x_ref[...]
    packed[tall:] = tile.astype(bf16)
    xg[i, j, :tall] = x_ref[...]
    xg[i, j, tall:] = tile.astype(bf16)

    sem = pltpu.get_barrier_semaphore()
    others = [(swap(i, t, n_dp), j) for t in range(1, n_dp)]
    others += [(i, lax.rem(j + u, n_hyper)) for u in range(1, n_hyper)]
    for dp, hyper in others:
        pl.semaphore_signal(sem, 1, device_id={"dp": dp, "hyper": hyper})
    pl.semaphore_wait(sem, len(others))

    na = n_dp // 2
    inp = Flood(xg, floods[:count], n_dp, half)
    inp.begin(packed)
    inp.across(0)
    inp.near(0)
    small = (emb_ref[...], hin_ref[...], hb_ref[...])
    diag_f[...] = spread(hypernet(xg[i, :, tall:, :], own, *small)[3])
    part[...] = jnp.zeros_like(part)
    get_w.wait()

    def forward(c, carry):
        slot = lax.rem(c, depth)
        buffer(c, slot).wait()
        for g in range(chunk // DG):
            rhs = bufs[slot, :, g * DG : (g + 1) * DG, :].reshape(hh * DG, classes)
            out = dot(diag_f[...], rhs).astype(bf16)
            heads_f[:, g * DG : (g + 1) * DG, :] = out.reshape(group, DG, classes)

        @pl.when(c + depth < chunks)
        def _():
            buffer(c + depth, slot).start()

        w = w_wide[:, pl.ds(pl.multiple_of(c * chunk, chunk), chunk)]
        bias = eb_ref[:, pl.ds(pl.multiple_of(j * wide + c * chunk, chunk), chunk)].astype(f32)
        for p in range(n_hyper):
            pre = dot(xg[i, p, :tall, :], w) + bias
            feat = (pre / (1.0 + jnp.exp(-pre))).astype(bf16)
            for s in range(own):
                part[p, s * rows : (s + 1) * rows, :] += dot(feat[s * rows : (s + 1) * rows], heads_f[p * own + s])
        return carry

    lax.fori_loop(0, chunks // 2, forward, 0)
    for t in range(1, na):
        inp.column(t)
    inp.pair(0)
    lax.fori_loop(chunks // 2, chunks, forward, 0)
    for t in range(1, na):
        inp.pair(t)
        inp.across(t)
    inp.corner(0)

    to_partner = {}
    for u in list(range(1, half)) + [0]:
        to_partner[u] = remote(
            part.at[lax.rem(partner + 2 * u, n_hyper)], from_partner.at[u], sp.at[u], rp.at[u], i, partner
        )
        to_partner[u].start()
    to_peer = {}
    for u in range(1, half):
        peer = lax.rem(j + 2 * u, n_hyper)
        to_partner[u].wait_recv()
        summed[u] = part[peer] + from_partner[u]
        to_peer[u] = remote(summed.at[u], from_peer.at[u], sq.at[u], rq.at[u], i, peer)
        to_peer[u].start()
    for t in range(1, na):
        inp.corner(t)
        inp.near(t)
    for t in range(na):
        inp.far(t)
    tiles = xg[:, :, tall:, :].reshape(n_dp * n_hyper, 16, width)
    select, picked, preact, hidden = hypernet(tiles, own, *small)
    select_out[...] = select
    picked_out[...] = picked
    pre_out[...] = preact
    hid_out[...] = hidden
    if aligned:
        get_n.wait()
        bias_n = eb_ref[:, pl.ds(pl.multiple_of(first, 128), narrow)].astype(f32)
        w_n = w_narrow
    else:
        bias_n = bn_ref[...].astype(f32)
        w_n = wn_ref

    nq = CS // group

    def prepare(base):
        mine = hid_out[pl.ds(pl.multiple_of(base * group, group), CS), :]
        diag[...] = spread(mine)

        def features(q, carry):
            for p in range(n_hyper):
                pre = dot(xg[base + q, p, :tall, :], w_n[...]) + bias_n
                logistic = 1.0 / (1.0 + jnp.exp(-pre))
                at = pl.ds(pl.multiple_of((q * n_hyper + p) * tall, tall), tall)
                feats[at, :] = (pre * logistic).astype(bf16)
                slopes[at, :] = logistic * (1.0 + pre * (1.0 - logistic))
            return carry

        lax.fori_loop(0, nq, features, 0)

    single = nq == n_dp
    if single:
        prepare(0)
    to_partner[0].wait_recv()
    logits = part[j] + from_partner[0]
    for u in range(1, half):
        to_peer[u].wait_recv()
        logits = logits + from_peer[u]
    eye = lax.broadcasted_iota(i32, (rows, rows), 0) == lax.broadcasted_iota(i32, (rows, rows), 1)
    columns = []
    for s in range(own):
        spot = jnp.where(eye, lab_ref[s : s + 1, :], 0)
        columns.append(jnp.sum(spot, axis=1, keepdims=True))
    label = jnp.concatenate(columns, axis=0)
    largest = jnp.max(logits, axis=-1, keepdims=True)
    exponent = jnp.exp(logits - largest)
    probability = exponent / jnp.sum(exponent, axis=-1, keepdims=True)
    onehot = (label == lax.broadcasted_iota(i32, logits.shape, 1)).astype(f32)
    dl = ((probability - onehot) / rows).astype(bf16)
    own_dl[...] = dl
    dl_all[i, j] = dl
    grads = Flood(dl_all, floods[count : 2 * count], n_dp, half)
    grads.begin(own_dl)

    gw_acc[...] = jnp.zeros_like(gw_acc)
    gb_acc[...] = jnp.zeros_like(gb_acc)

    def ho_group(g):
        return ho_n[:, pl.ds(pl.multiple_of(g * DG, DG), DG), :].reshape(hh * DG, classes)

    def heads_part(low, high):
        def step(g, carry):
            out = dot(diag[...], ho_group(g)).astype(bf16)
            heads[:, pl.ds(pl.multiple_of(g * DG, DG), DG), :] = out.reshape(CS, DG, classes)
            return carry

        lax.fori_loop(low, high, step, 0)

    def slots_part(base, low):
        def step(n, carry):
            q = low + n
            gw, gb = gw_acc[...], gb_acc[...]
            for p in range(n_hyper):
                block = (q - base) * n_hyper + p
                for s in range(own):
                    dl_s = dl_all[q, p, s * rows : (s + 1) * rows, :]
                    at = pl.ds(pl.multiple_of(block * tall + s * rows, rows), rows)
                    slot = (q * n_hyper + p) * own + s
                    dhead = dot(feats[at, :], dl_s, ((0,), (0,))).astype(bf16)
                    dheads[:, pl.ds(pl.multiple_of(slot * DG, DG), DG), :] = dhead.reshape(groups, DG, classes)
                    dfeat = dot(dl_s, heads[block * own + s], ((1,), (1,))).astype(bf16)
                    dpre[at, :] = (dfeat.astype(f32) * slopes[at, :]).astype(bf16)
            for p in range(n_hyper):
                block = (q - base) * n_hyper + p
                both = dpre[pl.ds(pl.multiple_of(block * tall, tall), tall), :]
                gw = gw + dot(xg[q, p, :tall, :], both, ((0,), (0,)))
                gb = gb + jnp.sum(both.astype(f32), axis=0, keepdims=True)
            gw_acc[...], gb_acc[...] = gw, gb
            return carry

        lax.fori_loop(0, 2, step, 0)

    def total_part(base, low, high):
        def step(g, carry):
            block = dheads[g, pl.ds(pl.multiple_of(base * group * DG, group * DG), CS * DG), :]
            total[...] += dot(block, ho_group(g), ((1,), (1,)))
            return carry

        lax.fori_loop(low, high, step, 0)

    def total_end(base):
        d = lax.broadcasted_iota(i32, total.shape, 0) % DG
        same = d == lax.broadcasted_iota(i32, total.shape, 1) % DG
        kept = jnp.sum(jnp.where(same, total[...], 0.0).reshape(CS, DG, hh * DG), axis=1)
        columns = lax.broadcasted_iota(i32, (hh * DG, 128), 0) // DG
        fold = (columns == lax.broadcasted_iota(i32, (hh * DG, 128), 1)).astype(f32)
        dh_mine[pl.ds(pl.multiple_of(base * group, group), CS), :] = dot(kept, fold, precision=highest)

    def flood_first(flood, work, count):
        cuts = [count * (t + 1) // na for t in range(na)]
        done = 0
        for t in range(1, na):
            work(done, cuts[t - 1])
            done = cuts[t - 1]
            flood.column(t)
            flood.pair(t - 1)
            flood.across(t - 1)
        flood.corner(0)
        work(done, count)
        flood.pair(na - 1)
        flood.across(na - 1)

    get_h.wait()
    if single:
        flood_first(grads, heads_part, groups)
        for t in range(na):
            if t + 1 < na:
                grads.corner(t + 1)
            grads.near(t)
            grads.far(t)
            slots_part(0, source(grads.a, t, na) * 2)
    else:
        flood_first(grads, lambda low, high: None, groups)
        for t in range(na):
            if t + 1 < na:
                grads.corner(t + 1)
            grads.near(t)
            grads.far(t)

        def one(q, carry):
            prepare(q * nq)
            heads_part(0, groups)
            for n in range(nq // 2):
                slots_part(q * nq, q * nq + 2 * n)
            total[...] = jnp.zeros_like(total)
            total_part(q * nq, 0, groups)
            total_end(q * nq)
            return carry

        lax.fori_loop(0, n_dp // nq, one, 0)
    put_heads = pltpu.make_async_copy(dheads, dheads_out, local_sems.at[3])
    put_heads.start()
    gw_own[:width] = gw_acc[...].astype(bf16)
    gw_own[width:] = jnp.broadcast_to(gb_acc[...], (16, narrow)).astype(bf16)
    if aligned:
        gw_all[i, j] = gw_own[...]
    else:
        put_own = pltpu.make_async_copy(gw_own, gw_all.at[i, j], local_sems.at[2])
        put_own.start()
        put_own.wait()
    fin = Flood(gw_all, floods[2 * count :], n_dp, half)
    fin.begin(gw_own)
    if single:
        total[...] = jnp.zeros_like(total)
        flood_first(fin, functools.partial(total_part, 0), groups)
        total_end(0)
    else:
        flood_first(fin, lambda low, high: None, groups)

    share = slots // n_hyper
    peers = [lax.rem(j + u, n_hyper) for u in range(1, n_hyper)]
    to_hyper = []
    for u in range(1, n_hyper):
        at = pl.ds(pl.multiple_of(peers[u - 1] * share, share), share)
        copy = remote(dh_mine.at[at], b1.at[u], sa.at[u], ra.at[u], i, peers[u - 1])
        copy.start()
        to_hyper.append(copy)
    for t in range(1, na):
        fin.corner(t)
    quarter = dh_mine[pl.ds(pl.multiple_of(j * share, share), share), :]
    for u in range(1, n_hyper):
        to_hyper[u - 1].wait_recv()
        quarter = quarter + b1[u]
    dh_sum[0] = quarter
    b2[i] = quarter
    to_dp = []
    for t in range(1, n_dp):
        copy = remote(dh_sum.at[0], b2.at[i], sb.at[t], rb.at[t], swap(i, t, n_dp), j)
        copy.start()
        to_dp.append(copy)
    for t in range(na):
        fin.near(t)
        fin.far(t)
    for copy in to_dp:
        copy.wait_recv()
    sum_all = b2[0]
    for t in range(1, n_dp):
        sum_all = sum_all + b2[t]
    dh_sum[1] = sum_all
    dh_all[j] = sum_all
    last = []
    for u in range(1, n_hyper):
        copy = remote(dh_sum.at[1], dh_all.at[j], sc.at[u], rc.at[u], i, peers[u - 1])
        copy.start()
        last.append(copy)
    for copy in last:
        copy.wait_recv()
    put_heads.wait()
    for copy in list(to_partner.values()) + list(to_peer.values()) + to_hyper + to_dp + last:
        copy.wait_send()
    for flood in (inp, grads, fin):
        flood.end()


def main_part(x, ids, labels, ew, eb, wn, bn, emb, hin_t, hb, ho, n_dp, n_hyper, aligned):
    own, rows = labels.shape
    tall, width = x.shape
    hh, wide, classes = ho.shape
    narrow = wide // n_dp
    half = n_hyper // 2
    group = n_hyper * own
    slots = group * n_dp
    CS = slots if slots <= 64 else 2 * group
    chunk = 128
    depth = 3 if slots <= 64 else 2
    block = tall + 16
    share = slots // n_hyper
    dma = pltpu.SemaphoreType.DMA
    sample = CS * rows
    vm = pltpu.VMEM
    ANY = pl.BlockSpec(memory_space=pl.ANY)
    shape = jax.ShapeDtypeStruct
    return pl.pallas_call(
        functools.partial(main_kernel, n_dp, half, own, rows, aligned),
        out_shape=(
            shape((n_dp, n_hyper, width + 16, narrow), bf16),
            shape((n_hyper, share, 128), f32),
            shape((narrow // DG, slots * DG, classes), bf16),
            shape((slots, hh), bf16),
            shape((slots, hh), f32),
            shape((slots, emb.shape[1]), bf16),
            shape((slots, emb.shape[0]), bf16),
        ),
        in_specs=[VM, pl.BlockSpec(memory_space=pltpu.SMEM), VM, ANY, VM, VM, VM, VM, VM, VM, ANY],
        out_specs=(VM if aligned else ANY, VM, ANY, VM, VM, VM, VM),
        scratch_shapes=[
            vm((block, width), bf16),
            vm((n_dp, n_hyper, block, width), bf16),
            vm((n_dp, n_hyper, tall, classes), bf16),
            vm((tall, classes), bf16),
            vm((width, wide), bf16),
            vm((width, narrow), bf16),
            vm((depth, hh, chunk, classes), bf16),
            vm((hh, narrow, classes), bf16),
            vm((group * DG, hh * DG), bf16),
            vm((group, chunk, classes), bf16),
            vm((n_hyper, tall, classes), f32),
            vm((half, tall, classes), f32),
            vm((half, tall, classes), f32),
            vm((half, tall, classes), f32),
            vm((CS * DG, hh * DG), bf16),
            vm((CS, narrow, classes), bf16),
            vm((narrow // DG, slots * DG, classes), bf16),
            vm((sample, narrow), bf16),
            vm((sample, narrow), f32),
            vm((sample, narrow), bf16),
            vm((CS * DG, hh * DG), f32),
            vm((width, narrow), f32),
            vm((1, narrow), f32),
            vm((width + 16, narrow), bf16),
            vm((slots, 128), f32),
            vm((n_hyper, share, 128), f32),
            vm((n_dp, share, 128), f32),
            vm((2, share, 128), f32),
            dma((4,)),
            dma((depth,)),
        ]
        + [dma((half,)) for _ in range(4)]
        + [dma((n_hyper,)), dma((n_hyper,)), dma((n_dp,)), dma((n_dp,)), dma((n_hyper,)), dma((n_hyper,))]
        + Flood.scratch(n_dp, half) * 3,
        compiler_params=pltpu.CompilerParams(
            collective_id=0, has_side_effects=True, vmem_limit_bytes=LIMIT
        ),
        name="main_part",
    )(x, ids, labels, ew, eb, wn, bn, emb, hin_t, hb, ho)


def last_kernel(aligned, dheads_ref, hid_ref, pre_ref, picked_ref, select_ref, hin_ref, dh_ref, gw_ref,
                go_ref, gwf_ref, gb_ref, table_ref, in_ref, hb_ref, diag_t):
    hh = go_ref.shape[0]
    classes = go_ref.shape[2]

    @pl.when(pl.program_id(0) == 0)
    def _():
        diag_t[...] = spread_t(hid_ref[...])
        dpre = dh_ref[...][:, :hh] * silu_slope(pre_ref[...])
        hb_ref[...] = jnp.sum(dpre, axis=0, keepdims=True)
        in_ref[...] = dot(dpre, picked_ref[...].astype(f32), ((0,), (0,)), precision=highest)
        back = dot(dpre, hin_ref[...].astype(f32), precision=highest)
        table_ref[...] = dot(select_ref[...].astype(f32), back, ((0,), (0,)), precision=highest)
        if aligned:
            n_dp, n_hyper, tall, narrow = gw_ref.shape
            for jj in range(n_hyper):
                for ii in range(n_dp):
                    at = (jj * n_dp + ii) * narrow
                    gwf_ref[:, at : at + narrow] = gw_ref[ii, jj, : tall - 16, :].astype(f32)
                    gb_ref[:, at : at + narrow] = gw_ref[ii, jj, tall - 16 : tall - 8, :].astype(f32)[:1]

    go_ref[...] = dot(diag_t[...], dheads_ref[0]).reshape(hh, DG, classes)


def last_part(dheads, hid, pre, picked, select, hin_t, dh, gw_all, aligned):
    groups, tall, classes = dheads.shape
    slots, hh = hid.shape
    width = picked.shape[1]
    clients = select.shape[1]
    n_dp, n_hyper, block, narrow = gw_all.shape
    whole = lambda *s: pl.BlockSpec(s, lambda g: (0,) * len(s))
    shape = jax.ShapeDtypeStruct
    full = (block - 16, n_dp * n_hyper * narrow) if aligned else (8, 128)
    bias = (1, full[1])
    given = gw_all if aligned else gw_all[:1, :1]
    return pl.pallas_call(
        functools.partial(last_kernel, aligned),
        grid=(groups,),
        out_shape=(
            shape((hh, groups * DG, classes), f32),
            shape(full, f32),
            shape(bias, f32),
            shape((clients, hin_t.shape[1]), f32),
            shape((hh, width), f32),
            shape((1, hh), f32),
        ),
        in_specs=[
            pl.BlockSpec((1, tall, classes), lambda g: (g, 0, 0)),
            whole(slots, hh), whole(slots, hh), whole(slots, width), whole(slots, clients),
            whole(*hin_t.shape), whole(slots, 128), whole(*given.shape),
        ],
        out_specs=[
            pl.BlockSpec((hh, DG, classes), lambda g: (0, g, 0)),
            whole(*full), whole(*bias), whole(clients, hin_t.shape[1]), whole(hh, width), whole(1, hh),
        ],
        scratch_shapes=[pltpu.VMEM((hh * DG, slots * DG), bf16)],
        compiler_params=pltpu.CompilerParams(vmem_limit_bytes=LIMIT),
        name="last_part",
    )(dheads, hid, pre, picked, select, hin_t, dh, given)


def local(
    inputs, labels, client_ids, ext_weight, ext_bias, embeddings, hyper_in, hyper_bias, hyper_out
):
    n_dp, n_hyper = lax.axis_size("dp"), lax.axis_size("hyper")
    own, rows, width = inputs.shape
    narrow = hyper_out.shape[0] // n_dp
    aligned = narrow % 128 == 0
    ho = hyper_out.transpose(1, 0, 2)
    hin_t = hyper_in.T
    bias = ext_bias[None]
    if aligned:
        wn, bn = jnp.zeros((8, 128), bf16), jnp.zeros((1, 128), bf16)
    else:
        start = (lax.axis_index("hyper") * n_dp + lax.axis_index("dp")) * narrow
        wn = lax.dynamic_slice_in_dim(ext_weight, start, narrow, 1)
        bn = lax.dynamic_slice_in_dim(bias, start, narrow, 1)
    gw_all, dh, dheads, hid, pre, picked, select = main_part(
        inputs.reshape(own * rows, width), client_ids, labels, ext_weight, bias, wn, bn,
        embeddings, hin_t, hyper_bias[None], ho, n_dp, n_hyper, aligned,
    )
    grad_out, gw, gb, table, grad_in, grad_hb = last_part(
        dheads, hid, pre, picked, select, hin_t, dh.reshape(-1, 128), gw_all, aligned
    )
    if not aligned:
        gw = gw_all[:, :, :width].transpose(2, 1, 0, 3).reshape(width, -1).astype(f32)
        gb = gw_all[:, :, width].transpose(1, 0, 2).reshape(-1).astype(f32)
    return (gw, gb.reshape(-1), table, grad_in.T, grad_hb.reshape(-1), grad_out.transpose(1, 0, 2))


def solution(mesh):
    placed = (
        P(("dp", "hyper"), None, None),
        P(("dp", "hyper"), None),
        P(("dp", "hyper")),
        P(),
        P(),
        P(),
        P(),
        P(),
        P("hyper", None, None),
    )
    return jax.shard_map(
        local,
        mesh=mesh,
        in_specs=placed,
        out_specs=(P(), P(), P(), P(), P(), P(("hyper", "dp"), None, None)),
        check_vma=False,
    )
```

```python
import functools

import jax
import jax.numpy as jnp
from jax import lax
from jax.experimental import pallas as pl
from jax.experimental.pallas import tpu as pltpu
from jax.sharding import PartitionSpec as P

highest = lax.Precision.HIGHEST
f32 = jnp.float32
bf16 = jnp.bfloat16
i32 = jnp.int32
VM = pl.BlockSpec(memory_space=pltpu.VMEM)
DG = 16
LIMIT = 60 * 1024 * 1024


def silu_slope(values):
    logistic = jax.nn.sigmoid(values)
    return logistic * (1.0 + values * (1.0 - logistic))


def dot(a, b, dims=((1,), (0,)), **kw):
    return lax.dot_general(a, b, (dims, ((), ())), preferred_element_type=f32, **kw)


def swap(index, other, count):
    if count & (count - 1):
        return lax.rem(index + other, count)
    out = index
    bit = 1
    while bit < count:
        if other & bit:
            out = out + bit - 2 * bit * lax.rem(index // bit, 2)
        bit *= 2
    return out


def source(index, other, count):
    if count & (count - 1):
        return lax.rem(index + count - other, count)
    return swap(index, other, count)


def place():
    i, j = lax.axis_index("dp"), lax.axis_index("hyper")
    return i, j, j + 1 - 2 * lax.rem(j, 2)


def spread(hidden):
    k, h = hidden.shape
    rows = lax.broadcasted_iota(i32, (k * DG, k), 0) // DG
    pick = (rows == lax.broadcasted_iota(i32, (k * DG, k), 1)).astype(bf16)
    tall = dot(pick, hidden).astype(bf16)
    columns = lax.broadcasted_iota(i32, (h, h * DG), 1) // DG
    widen = (columns == lax.broadcasted_iota(i32, (h, h * DG), 0)).astype(bf16)
    full = dot(tall, widen)
    d = lax.broadcasted_iota(i32, full.shape, 0) % DG
    same = d == lax.broadcasted_iota(i32, full.shape, 1) % DG
    return jnp.where(same, full, 0.0).astype(bf16)


def spread_t(hidden):
    k, h = hidden.shape
    rows = lax.broadcasted_iota(i32, (h * DG, h), 0) // DG
    pick = (rows == lax.broadcasted_iota(i32, (h * DG, h), 1)).astype(bf16)
    tall = dot(pick, hidden, ((1,), (1,))).astype(bf16)
    columns = lax.broadcasted_iota(i32, (k, k * DG), 1) // DG
    widen = (columns == lax.broadcasted_iota(i32, (k, k * DG), 0)).astype(bf16)
    full = dot(tall, widen)
    d = lax.broadcasted_iota(i32, full.shape, 0) % DG
    same = d == lax.broadcasted_iota(i32, full.shape, 1) % DG
    return jnp.where(same, full, 0.0).astype(bf16)


def remote(src, dst, send, recv, dp, hyper):
    return pltpu.make_async_remote_copy(
        src_ref=src, dst_ref=dst, send_sem=send, recv_sem=recv, device_id={"dp": dp, "hyper": hyper}
    )


class Flood:
    def __init__(self, out, sems, n_dp, half):
        self.out, self.sems = out, sems
        self.na, self.half, self.n_hyper = n_dp // 2, half, 2 * half
        self.i, self.j, self.partner = place()
        self.a, self.b = self.i // 2, lax.rem(self.i, 2)
        self.cut = out.shape[2] // 32 * 16
        self.tall = out.shape[2]
        self.copies = {}

    @staticmethod
    def scratch(n_dp, half):
        dma, na = pltpu.SemaphoreType.DMA, n_dp // 2
        shapes = [(na,), (na,), (na, half), (na, half), (na, half), (na, 2, half)]
        return [dma(s) for s in shapes for _ in range(2)]

    def at(self, t, b, u):
        dp = source(self.a, t, self.na) * 2 + (self.b if b == 0 else 1 - self.b)
        return dp, lax.rem(self.j + self.n_hyper - 2 * u, self.n_hyper)

    def send(self, kind, index, block, where, dp, hyper, rows=None):
        number = "zxypqc".index(kind)
        s, r = self.sems[2 * number], self.sems[2 * number + 1]
        target = self.out.at[where[0], where[1]]
        if rows is not None:
            block, target = block.at[pl.ds(*rows)], target.at[pl.ds(*rows)]
        copy = remote(block, target, s.at[index], r.at[index], dp, hyper)
        copy.start()
        self.copies[kind, index] = copy

    def recv(self, kind, index):
        self.copies[kind, index].wait_recv()

    def peers(self):
        return [(u, lax.rem(self.j + 2 * u, self.n_hyper)) for u in range(1, self.half)]

    def column(self, t, own=None):
        where = self.at(t, 0, 0)
        if t:
            self.recv("z", (t,))
        block = self.out.at[where[0], where[1]] if own is None else own
        for u, peer in self.peers():
            self.send("y", (t, u), block, where, self.i, peer)
        self.send("x", (t,), block, where, self.a * 2 + 1 - self.b, self.j)
        self.send("c", (t, 0, 0), block, where, self.i, self.partner)

    def begin(self, own):
        where = self.at(0, 0, 0)
        for t in range(1, self.na):
            self.send("z", (t,), own, where, swap(self.a, t, self.na) * 2 + self.b, self.j)
        self.column(0, own)

    def pair(self, t):
        where = self.at(t, 1, 0)
        self.recv("x", (t,))
        block = self.out.at[where[0], where[1]]
        for u, peer in self.peers():
            self.send("p", (t, u), block, where, self.i, peer, (0, self.cut))
        self.send("c", (t, 1, 0), block, where, self.i, self.partner)

    def across(self, t):
        for u, peer in self.peers():
            where = self.at(t, 0, u)
            self.recv("y", (t, u))
            block = self.out.at[where[0], where[1]]
            self.send("c", (t, 0, u), block, where, self.i, self.partner)
            self.send(
                "q", (t, u), block, where, self.a * 2 + 1 - self.b, self.j, (self.cut, self.tall - self.cut)
            )

    def corner(self, t):
        for u, peer in self.peers():
            where = self.at(t, 1, u)
            self.recv("p", (t, u))
            self.recv("q", (t, u))
            self.send("c", (t, 1, u), self.out.at[where[0], where[1]], where, self.i, self.partner)

    def near(self, t):
        for u in range(self.half):
            self.recv("c", (t, 0, u))

    def far(self, t):
        for u in range(self.half):
            self.recv("c", (t, 1, u))

    def end(self):
        for copy in self.copies.values():
            copy.wait_send()


def hypernet(tiles, own, emb, hin_t, hb):
    blocks = tiles.shape[0]
    tiles = tiles.astype(f32)
    ids = (tiles[:, :8] * 256.0 + tiles[:, 8:]).reshape(blocks * 8, tiles.shape[2])[:, :1]
    clients = emb.shape[0]
    wide = (ids == lax.broadcasted_iota(i32, (blocks * 8, clients), 1).astype(f32)).astype(f32).astype(bf16)
    slots = blocks * own
    row = lax.broadcasted_iota(i32, (slots, blocks * 8), 0)
    column = lax.broadcasted_iota(i32, (slots, blocks * 8), 1)
    keep = (column == row // own * 8 + row % own).astype(f32).astype(bf16)
    select = dot(keep, wide).astype(bf16)
    picked = dot(select, emb).astype(bf16)
    preact = dot(picked, hin_t, ((1,), (1,))) + hb
    hidden = (preact / (1.0 + jnp.exp(-preact))).astype(bf16)
    return select, picked, preact, hidden


def main_kernel(
    n_dp, half, own, rows, aligned,
    x_ref, ids_ref, lab_ref, ew_ref, eb_ref, wn_ref, bn_ref, emb_ref, hin_ref, hb_ref, ho_ref,
    gw_all, dh_all, go_out, pre_out, picked_out, select_out,
    packed, xg, dl_all, own_dl, w_wide, w_narrow, bufs, ho_n, diag_f, heads_f, part,
    from_partner, summed, from_peer, diag, heads, dheads, diag_t, go, go_acc, feats, slopes, dpre,
    gw_acc, gb_acc, gw_own, dh_mine, b1, b2, dh_sum, hid_out, bias_w, id_own, id_all, local_sems, buf_sems,
    sp, rp, sq, rq, si, ri, sa, ra, sb, rb, sc, rc, *floods
):
    count = len(floods) // 3
    i, j, partner = place()
    n_hyper = 2 * half
    tall, width = x_ref.shape
    hh, wide, classes = ho_ref.shape
    chunk = bufs.shape[2]
    chunks = wide // chunk
    narrow = wide // n_dp
    groups = narrow // DG
    depth = bufs.shape[0]
    slots = n_dp * n_hyper * own
    group = n_hyper * own
    CS = diag.shape[0] // DG

    def buffer(c, slot):
        at = pl.ds(pl.multiple_of(c * chunk, chunk), chunk)
        return pltpu.make_async_copy(ho_ref.at[:, at, :], bufs.at[slot], buf_sems.at[slot])

    for c in range(min(depth, chunks)):
        buffer(c, c).start()
    wide_at = pl.ds(pl.multiple_of(j * wide, 128), wide)
    get_w = pltpu.make_async_copy(ew_ref.at[:, wide_at], w_wide, local_sems.at[0])
    get_w.start()
    get_h = pltpu.make_async_copy(
        ho_ref.at[:, pl.ds(pl.multiple_of(i * narrow, narrow), narrow), :], ho_n, local_sems.at[1]
    )
    get_h.start()
    first = (j * n_dp + i) * narrow
    if aligned:
        narrow_at = pl.ds(pl.multiple_of(first, 128), narrow)
        get_n = pltpu.make_async_copy(ew_ref.at[:, narrow_at], w_narrow, local_sems.at[2])
        get_n.start()

    row = lax.broadcasted_iota(i32, (16, width), 0)
    tile = jnp.zeros((16, width), f32)
    for s in range(own):
        number = ids_ref[s]
        tile = jnp.where(row == s, (number // 256).astype(f32), tile)
        tile = jnp.where(row == 8 + s, (number % 256).astype(f32), tile)
    packed[:tall] = x_ref[...]
    packed[tall:] = tile.astype(bf16)
    id_own[...] = tile.astype(bf16)
    id_all[j] = tile.astype(bf16)
    xg[i, j, :tall] = x_ref[...]
    xg[i, j, tall:] = tile.astype(bf16)

    sem = pltpu.get_barrier_semaphore()
    others = [(swap(i, t, n_dp), j) for t in range(1, n_dp)]
    others += [(i, lax.rem(j + u, n_hyper)) for u in range(1, n_hyper)]
    for dp, hyper in others:
        pl.semaphore_signal(sem, 1, device_id={"dp": dp, "hyper": hyper})
    pl.semaphore_wait(sem, len(others))

    na = n_dp // 2
    inp = Flood(xg, floods[:count], n_dp, half)
    to_ids = []
    for u in range(1, n_hyper):
        copy = remote(id_own, id_all.at[j], si.at[u], ri.at[u], i, lax.rem(j + u, n_hyper))
        copy.start()
        to_ids.append(copy)
    inp.begin(packed)
    for copy in to_ids:
        copy.wait_recv()
    small = (emb_ref[...], hin_ref[...], hb_ref[...])
    diag_f[...] = spread(hypernet(id_all[...], own, *small)[3])
    part[...] = jnp.zeros_like(part)
    bias_w[...] = eb_ref[pl.ds(pl.multiple_of(j * wide, 256), wide)].astype(f32)[None]
    get_w.wait()
    inp.across(0)
    inp.near(0)

    def forward(c, carry):
        slot = lax.rem(c, depth)
        buffer(c, slot).wait()
        for g in range(chunk // DG):
            rhs = bufs[slot, :, g * DG : (g + 1) * DG, :].reshape(hh * DG, classes)
            out = dot(diag_f[...], rhs).astype(bf16)
            heads_f[:, g * DG : (g + 1) * DG, :] = out.reshape(group, DG, classes)

        @pl.when(c + depth < chunks)
        def _():
            buffer(c + depth, slot).start()

        w = w_wide[:, pl.ds(pl.multiple_of(c * chunk, chunk), chunk)]
        bias = bias_w[:, pl.ds(pl.multiple_of(c * chunk, chunk), chunk)]
        for p in range(n_hyper):
            pre = dot(xg[i, p, :tall, :], w) + bias
            feat = (pre / (1.0 + jnp.exp(-pre))).astype(bf16)
            for s in range(own):
                part[p, s * rows : (s + 1) * rows, :] += dot(feat[s * rows : (s + 1) * rows], heads_f[p * own + s])
        return carry

    lax.fori_loop(0, chunks // 2, forward, 0)
    for t in range(1, na):
        inp.column(t)
    inp.pair(0)
    lax.fori_loop(chunks // 2, chunks, forward, 0)
    for t in range(1, na):
        inp.pair(t)
        inp.across(t)
    inp.corner(0)

    to_partner = {}
    for u in list(range(1, half)) + [0]:
        to_partner[u] = remote(
            part.at[lax.rem(partner + 2 * u, n_hyper)], from_partner.at[u], sp.at[u], rp.at[u], i, partner
        )
        to_partner[u].start()
    to_peer = {}
    for u in range(1, half):
        peer = lax.rem(j + 2 * u, n_hyper)
        to_partner[u].wait_recv()
        summed[u] = part[peer] + from_partner[u]
        to_peer[u] = remote(summed.at[u], from_peer.at[u], sq.at[u], rq.at[u], i, peer)
        to_peer[u].start()
    for t in range(1, na):
        inp.corner(t)
        inp.near(t)
    for t in range(na):
        inp.far(t)
    tiles = xg[:, :, tall:, :].reshape(n_dp * n_hyper, 16, width)
    select, picked, preact, hidden = hypernet(tiles, own, *small)
    select_out[...] = select
    picked_out[...] = picked
    pre_out[...] = preact
    hid_out[...] = hidden
    if aligned:
        get_n.wait()
        bias_n = bias_w[:, pl.ds(pl.multiple_of(i * narrow, 128), narrow)]
        w_n = w_narrow
    else:
        bias_n = bn_ref[...].astype(f32)
        w_n = wn_ref

    nq = CS // group

    def prepare(base):
        mine = hid_out[pl.ds(pl.multiple_of(base * group, group), CS), :]
        diag[...] = spread(mine)

        def features(q, carry):
            for p in range(n_hyper):
                pre = dot(xg[base + q, p, :tall, :], w_n[...]) + bias_n
                logistic = 1.0 / (1.0 + jnp.exp(-pre))
                at = pl.ds(pl.multiple_of((q * n_hyper + p) * tall, tall), tall)
                feats[at, :] = (pre * logistic).astype(bf16)
                slopes[at, :] = logistic * (1.0 + pre * (1.0 - logistic))
            return carry

        lax.fori_loop(0, nq, features, 0)

    single = nq == n_dp
    if single:
        prepare(0)
        diag_t[...] = spread_t(hidden)
    to_partner[0].wait_recv()
    logits = part[j] + from_partner[0]
    for u in range(1, half):
        to_peer[u].wait_recv()
        logits = logits + from_peer[u]
    eye = lax.broadcasted_iota(i32, (rows, rows), 0) == lax.broadcasted_iota(i32, (rows, rows), 1)
    columns = []
    for s in range(own):
        spot = jnp.where(eye, lab_ref[s : s + 1, :], 0)
        columns.append(jnp.sum(spot, axis=1, keepdims=True))
    label = jnp.concatenate(columns, axis=0)
    largest = jnp.max(logits, axis=-1, keepdims=True)
    exponent = jnp.exp(logits - largest)
    probability = exponent / jnp.sum(exponent, axis=-1, keepdims=True)
    onehot = (label == lax.broadcasted_iota(i32, logits.shape, 1)).astype(f32)
    dl = ((probability - onehot) / rows).astype(bf16)
    own_dl[...] = dl
    dl_all[i, j] = dl
    grads = Flood(dl_all, floods[count : 2 * count], n_dp, half)
    grads.begin(own_dl)

    gw_acc[...] = jnp.zeros_like(gw_acc)
    gb_acc[...] = jnp.zeros_like(gb_acc)

    def ho_group(g):
        return ho_n[:, pl.ds(pl.multiple_of(g * DG, DG), DG), :].reshape(hh * DG, classes)

    def heads_part(low, high):
        def step(g, carry):
            out = dot(diag[...], ho_group(g)).astype(bf16)
            heads[:, pl.ds(pl.multiple_of(g * DG, DG), DG), :] = out.reshape(CS, DG, classes)
            return carry

        lax.fori_loop(low, high, step, 0)

    def slots_part(base, low):
        def step(n, carry):
            q = low + n
            gw, gb = gw_acc[...], gb_acc[...]
            for p in range(n_hyper):
                block = (q - base) * n_hyper + p
                for s in range(own):
                    dl_s = dl_all[q, p, s * rows : (s + 1) * rows, :]
                    at = pl.ds(pl.multiple_of(block * tall + s * rows, rows), rows)
                    slot = (q * n_hyper + p) * own + s
                    dhead = dot(feats[at, :], dl_s, ((0,), (0,))).astype(bf16)
                    dheads[:, pl.ds(pl.multiple_of(slot * DG, DG), DG), :] = dhead.reshape(groups, DG, classes)
                    dfeat = dot(dl_s, heads[block * own + s], ((1,), (1,))).astype(bf16)
                    dpre[at, :] = (dfeat.astype(f32) * slopes[at, :]).astype(bf16)
            for p in range(n_hyper):
                block = (q - base) * n_hyper + p
                both = dpre[pl.ds(pl.multiple_of(block * tall, tall), tall), :]
                gw = gw + dot(xg[q, p, :tall, :], both, ((0,), (0,)))
                gb = gb + jnp.sum(both.astype(f32), axis=0, keepdims=True)
            gw_acc[...], gb_acc[...] = gw, gb
            return carry

        lax.fori_loop(0, 2, step, 0)

    def go_part(low, high):
        def step(g, carry):
            at = pl.ds(pl.multiple_of(g * DG, DG), DG)
            go[:, at, :] = dot(diag_t[...], dheads[g]).astype(bf16).reshape(hh, DG, classes)
            return carry

        if single:
            lax.fori_loop(low, high, step, 0)

    def total_part(q0):
        count = 2 * group * DG
        at = pl.ds(pl.multiple_of(q0 * group * DG, group * DG), count)
        z = dot(ho_group(0), dheads[0, at, :], ((1,), (1,)))
        for g in range(1, groups):
            z = z + dot(ho_group(g), dheads[g, at, :], ((1,), (1,)))
        d = lax.broadcasted_iota(i32, z.shape, 0) % DG
        same = d == lax.broadcasted_iota(i32, z.shape, 1) % DG
        kept = jnp.sum(jnp.where(same, z, 0.0).reshape(hh, DG, count), axis=1)
        kept = jnp.concatenate([kept, jnp.zeros((128 - hh, count), f32)], axis=0)
        fold = lax.broadcasted_iota(i32, (2 * group, count), 1) // DG
        fold = (fold == lax.broadcasted_iota(i32, (2 * group, count), 0)).astype(f32)
        mine = dot(fold, kept, ((1,), (1,)), precision=highest)
        dh_mine[pl.ds(pl.multiple_of(q0 * group, group), 2 * group), :] = mine

    def flood_first(flood, work, count):
        cuts = [count * (t + 1) // na for t in range(na)]
        done = 0
        for t in range(1, na):
            work(done, cuts[t - 1])
            done = cuts[t - 1]
            flood.column(t)
            flood.pair(t - 1)
            flood.across(t - 1)
        flood.corner(0)
        work(done, count)
        flood.pair(na - 1)
        flood.across(na - 1)

    get_h.wait()
    if single:
        flood_first(grads, heads_part, groups)
        for t in range(na):
            if t + 1 < na:
                grads.corner(t + 1)
            grads.near(t)
            grads.far(t)
            slots_part(0, source(grads.a, t, na) * 2)
            if t + 1 < na:
                total_part(source(grads.a, t, na) * 2)
    else:
        flood_first(grads, lambda low, high: None, groups)
        for t in range(na):
            if t + 1 < na:
                grads.corner(t + 1)
            grads.near(t)
            grads.far(t)

        def one(q, carry):
            prepare(q * nq)
            heads_part(0, groups)
            for n in range(nq // 2):
                slots_part(q * nq, q * nq + 2 * n)
            for n in range(nq // 2):
                total_part(q * nq + 2 * n)
            diag_t[...] = spread_t(hid_out[pl.ds(pl.multiple_of(q * CS, CS), CS), :])
            at = pl.ds(pl.multiple_of(q * CS * DG, CS * DG), CS * DG)
            for g in range(groups):
                spot = slice(g * DG, (g + 1) * DG)
                go_acc[:, spot, :] += dot(diag_t[...], dheads[g, at, :]).reshape(hh, DG, classes)
            return carry

        go_acc[...] = jnp.zeros_like(go_acc)

        lax.fori_loop(0, n_dp // nq, one, 0)
        go[...] = go_acc[...].astype(bf16)
    gw_own[:width] = gw_acc[...].astype(bf16)
    gw_own[width:] = jnp.broadcast_to(gb_acc[...], (16, narrow)).astype(bf16)
    if aligned:
        gw_all[i, j] = gw_own[...]
    else:
        put_own = pltpu.make_async_copy(gw_own, gw_all.at[i, j], local_sems.at[2])
        put_own.start()
        put_own.wait()
    fin = Flood(gw_all, floods[2 * count :], n_dp, half)
    fin.begin(gw_own)
    if single:
        total_part(source(grads.a, na - 1, na) * 2)

    share = slots // n_hyper
    peers = [lax.rem(j + u, n_hyper) for u in range(1, n_hyper)]
    to_hyper = []
    for u in range(1, n_hyper):
        at = pl.ds(pl.multiple_of(peers[u - 1] * share, share), share)
        copy = remote(dh_mine.at[at], b1.at[u], sa.at[u], ra.at[u], i, peers[u - 1])
        copy.start()
        to_hyper.append(copy)
    quart = groups // 4
    go_part(0, quart)
    fin.column(1)
    fin.pair(0)
    fin.across(0)
    quarter = dh_mine[pl.ds(pl.multiple_of(j * share, share), share), :]
    for u in range(1, n_hyper):
        to_hyper[u - 1].wait_recv()
        quarter = quarter + b1[u]
    dh_sum[0] = quarter
    b2[i] = quarter
    to_dp = []
    for t in range(1, n_dp):
        copy = remote(dh_sum.at[0], b2.at[i], sb.at[t], rb.at[t], swap(i, t, n_dp), j)
        copy.start()
        to_dp.append(copy)
    go_part(quart, 2 * quart)
    for t in range(2, na):
        fin.column(t)
        fin.pair(t - 1)
        fin.across(t - 1)
    fin.corner(0)
    go_part(2 * quart, 3 * quart)
    for copy in to_dp:
        copy.wait_recv()
    sum_all = b2[0]
    for t in range(1, n_dp):
        sum_all = sum_all + b2[t]
    dh_sum[1] = sum_all
    dh_all[j] = sum_all
    last = []
    for u in range(1, n_hyper):
        copy = remote(dh_sum.at[1], dh_all.at[j], sc.at[u], rc.at[u], i, peers[u - 1])
        copy.start()
        last.append(copy)
    fin.pair(na - 1)
    fin.across(na - 1)
    go_part(3 * quart, groups)
    put_go = pltpu.make_async_copy(go, go_out, local_sems.at[3])
    put_go.start()
    for t in range(1, na):
        fin.corner(t)
    for t in range(na):
        fin.near(t)
        fin.far(t)
    for copy in last:
        copy.wait_recv()
    put_go.wait()
    for copy in list(to_partner.values()) + list(to_peer.values()) + to_hyper + to_dp + last + to_ids:
        copy.wait_send()
    for flood in (inp, grads, fin):
        flood.end()


def main_part(x, ids, labels, ew, eb, wn, bn, emb, hin_t, hb, ho, n_dp, n_hyper, aligned):
    own, rows = labels.shape
    tall, width = x.shape
    hh, wide, classes = ho.shape
    narrow = wide // n_dp
    half = n_hyper // 2
    group = n_hyper * own
    slots = group * n_dp
    CS = slots if slots <= 64 else 2 * group
    chunk = 128
    depth = 3 if slots <= 64 else 2
    block = tall + 16
    share = slots // n_hyper
    dma = pltpu.SemaphoreType.DMA
    sample = CS * rows
    vm = pltpu.VMEM
    ANY = pl.BlockSpec(memory_space=pl.ANY)
    shape = jax.ShapeDtypeStruct
    return pl.pallas_call(
        functools.partial(main_kernel, n_dp, half, own, rows, aligned),
        out_shape=(
            shape((n_dp, n_hyper, width + 16, narrow), bf16),
            shape((n_hyper, share, 128), f32),
            shape((hh, narrow, classes), bf16),
            shape((slots, hh), f32),
            shape((slots, emb.shape[1]), bf16),
            shape((slots, emb.shape[0]), bf16),
        ),
        in_specs=[VM, pl.BlockSpec(memory_space=pltpu.SMEM), VM, ANY, VM, VM, VM, VM, VM, VM, ANY],
        out_specs=(VM if aligned else ANY, VM, ANY, VM, VM, VM),
        scratch_shapes=[
            vm((block, width), bf16),
            vm((n_dp, n_hyper, block, width), bf16),
            vm((n_dp, n_hyper, tall, classes), bf16),
            vm((tall, classes), bf16),
            vm((width, wide), bf16),
            vm((width, narrow), bf16),
            vm((depth, hh, chunk, classes), bf16),
            vm((hh, narrow, classes), bf16),
            vm((group * DG, hh * DG), bf16),
            vm((group, chunk, classes), bf16),
            vm((n_hyper, tall, classes), f32),
            vm((half, tall, classes), f32),
            vm((half, tall, classes), f32),
            vm((half, tall, classes), f32),
            vm((CS * DG, hh * DG), bf16),
            vm((CS, narrow, classes), bf16),
            vm((narrow // DG, slots * DG, classes), bf16),
            vm((hh * DG, CS * DG), bf16),
            vm((hh, narrow, classes), bf16),
            vm((8, 8, 128) if CS == slots else (hh, narrow, classes), f32),
            vm((sample, narrow), bf16),
            vm((sample, narrow), f32),
            vm((sample, narrow), bf16),
            vm((width, narrow), f32),
            vm((1, narrow), f32),
            vm((width + 16, narrow), bf16),
            vm((slots, 128), f32),
            vm((n_hyper, share, 128), f32),
            vm((n_dp, share, 128), f32),
            vm((2, share, 128), f32),
            vm((slots, hh), bf16),
            vm((1, wide), f32),
            vm((16, width), bf16),
            vm((n_hyper, 16, width), bf16),
            dma((4,)),
            dma((depth,)),
        ]
        + [dma((half,)) for _ in range(4)]
        + [dma((n_hyper,)), dma((n_hyper,))]
        + [dma((n_hyper,)), dma((n_hyper,)), dma((n_dp,)), dma((n_dp,)), dma((n_hyper,)), dma((n_hyper,))]
        + Flood.scratch(n_dp, half) * 3,
        compiler_params=pltpu.CompilerParams(
            collective_id=0, has_side_effects=True, vmem_limit_bytes=LIMIT
        ),
        name="main_part",
    )(x, ids, labels, ew, eb, wn, bn, emb, hin_t, hb, ho)


def last_kernel(aligned, go_ref, pre_ref, picked_ref, select_ref, hin_ref, dh_ref, gw_ref,
                go_out, gwf_out, gb_ref, table_ref, in_ref, hb_ref, gwf_ref, sem):
    hh = go_ref.shape[0]
    last = pl.num_programs(0) - 1

    @pl.when(pl.program_id(0) == jnp.minimum(1, last))
    def _():
        if aligned:
            n_dp, n_hyper, tall, narrow = gw_ref.shape
            for jj in range(n_hyper):
                for ii in range(n_dp):
                    at = (jj * n_dp + ii) * narrow
                    gwf_ref[:, at : at + narrow] = gw_ref[ii, jj, : tall - 16, :].astype(f32)
                    gb_ref[:, at : at + narrow] = gw_ref[ii, jj, tall - 16 : tall - 8, :].astype(f32)[:1]
            pltpu.make_async_copy(gwf_ref, gwf_out, sem).start()

    @pl.when(pl.program_id(0) == jnp.minimum(2, last))
    def _():
        dpre = dh_ref[...][:, :hh] * silu_slope(pre_ref[...])
        hb_ref[...] = jnp.sum(dpre, axis=0, keepdims=True)
        in_ref[...] = dot(dpre, picked_ref[...].astype(f32), ((0,), (0,)), precision=highest)
        back = dot(dpre, hin_ref[...].astype(f32), precision=highest)
        table_ref[...] = dot(select_ref[...].astype(f32), back, ((0,), (0,)), precision=highest)

    go_out[...] = go_ref[...].astype(f32)

    @pl.when(pl.program_id(0) == last)
    def _():
        if aligned:
            pltpu.make_async_copy(gwf_ref, gwf_out, sem).wait()


def last_part(go, pre, picked, select, hin_t, dh, gw_all, aligned):
    hh, wide, classes = go.shape
    slots, width = picked.shape
    clients = select.shape[1]
    n_dp, n_hyper, block, narrow = gw_all.shape
    whole = lambda *s: pl.BlockSpec(s, lambda g: (0,) * len(s))
    shape = jax.ShapeDtypeStruct
    full = (block - 16, n_dp * n_hyper * narrow) if aligned else (8, 128)
    bias = (1, full[1])
    given = gw_all if aligned else gw_all[:1, :1]
    per = 32 if wide % 32 == 0 else wide
    cut = pl.BlockSpec((hh, per, classes), lambda g: (0, g, 0))
    return pl.pallas_call(
        functools.partial(last_kernel, aligned),
        grid=(wide // per,),
        out_shape=(
            shape(go.shape, f32),
            shape(full, f32),
            shape(bias, f32),
            shape((clients, hin_t.shape[1]), f32),
            shape((hh, width), f32),
            shape((1, hh), f32),
        ),
        in_specs=[
            cut, whole(slots, hh), whole(slots, width), whole(slots, clients),
            whole(*hin_t.shape), whole(slots, 128), whole(*given.shape),
        ],
        out_specs=[
            cut, pl.BlockSpec(memory_space=pl.ANY),
            whole(*bias), whole(clients, hin_t.shape[1]), whole(hh, width), whole(1, hh),
        ],
        scratch_shapes=[pltpu.VMEM(full, f32), pltpu.SemaphoreType.DMA],
        compiler_params=pltpu.CompilerParams(vmem_limit_bytes=LIMIT),
        name="last_part",
    )(go, pre, picked, select, hin_t, dh, given)


def local(
    inputs, labels, client_ids, ext_weight, ext_bias, embeddings, hyper_in, hyper_bias, hyper_out
):
    n_dp, n_hyper = lax.axis_size("dp"), lax.axis_size("hyper")
    own, rows, width = inputs.shape
    narrow = hyper_out.shape[0] // n_dp
    aligned = narrow % 128 == 0
    ho = hyper_out.transpose(1, 0, 2)
    hin_t = hyper_in.T
    bias = ext_bias
    if aligned:
        wn, bn = embeddings, hyper_bias[None]
    else:
        start = (lax.axis_index("hyper") * n_dp + lax.axis_index("dp")) * narrow
        wn = lax.dynamic_slice_in_dim(ext_weight, start, narrow, 1)
        bn = lax.dynamic_slice_in_dim(bias, start, narrow, 0)[None]
    gw_all, dh, go, pre, picked, select = main_part(
        inputs.reshape(own * rows, width), client_ids, labels, ext_weight, bias, wn, bn,
        embeddings, hin_t, hyper_bias[None], ho, n_dp, n_hyper, aligned,
    )
    grad_out, gw, gb, table, grad_in, grad_hb = last_part(
        go, pre, picked, select, hin_t, dh.reshape(-1, 128), gw_all, aligned
    )
    if not aligned:
        gw = gw_all[:, :, :width].transpose(2, 1, 0, 3).reshape(width, -1).astype(f32)
        gb = gw_all[:, :, width].transpose(1, 0, 2).reshape(-1).astype(f32)
    return (gw, gb.reshape(-1), table, grad_in.T, grad_hb.reshape(-1), grad_out.transpose(1, 0, 2))


def solution(mesh):
    placed = (
        P(("dp", "hyper"), None, None),
        P(("dp", "hyper"), None),
        P(("dp", "hyper")),
        P(),
        P(),
        P(),
        P(),
        P(),
        P("hyper", None, None),
    )
    return jax.shard_map(
        local,
        mesh=mesh,
        in_specs=placed,
        out_specs=(P(), P(), P(), P(), P(), P(("hyper", "dp"), None, None)),
        check_vma=False,
    )
```

```python
import functools

import jax
import jax.numpy as jnp
from jax import lax
from jax.experimental import pallas as pl
from jax.experimental.pallas import tpu as pltpu
from jax.sharding import PartitionSpec as P

highest = lax.Precision.HIGHEST
f32 = jnp.float32
bf16 = jnp.bfloat16
i32 = jnp.int32
VM = pl.BlockSpec(memory_space=pltpu.VMEM)
DG = 16
HG = 8
LIMIT = 60 * 1024 * 1024


def silu_slope(values):
    logistic = jax.nn.sigmoid(values)
    return logistic * (1.0 + values * (1.0 - logistic))


def dot(a, b, dims=((1,), (0,)), **kw):
    return lax.dot_general(a, b, (dims, ((), ())), preferred_element_type=f32, **kw)


def swap(index, other, count):
    if count & (count - 1):
        return lax.rem(index + other, count)
    out = index
    bit = 1
    while bit < count:
        if other & bit:
            out = out + bit - 2 * bit * lax.rem(index // bit, 2)
        bit *= 2
    return out


def source(index, other, count):
    if count & (count - 1):
        return lax.rem(index + count - other, count)
    return swap(index, other, count)


def place():
    i, j = lax.axis_index("dp"), lax.axis_index("hyper")
    return i, j, j + 1 - 2 * lax.rem(j, 2)


def spread(hidden):
    k, h = hidden.shape
    rows = lax.broadcasted_iota(i32, (k * HG, k), 0) // HG
    pick = (rows == lax.broadcasted_iota(i32, (k * HG, k), 1)).astype(bf16)
    tall = dot(pick, hidden).astype(bf16)
    columns = lax.broadcasted_iota(i32, (h, h * HG), 1) // HG
    widen = (columns == lax.broadcasted_iota(i32, (h, h * HG), 0)).astype(bf16)
    full = dot(tall, widen)
    d = lax.broadcasted_iota(i32, full.shape, 0) % HG
    same = d == lax.broadcasted_iota(i32, full.shape, 1) % HG
    return jnp.where(same, full, 0.0).astype(bf16)


def halves(tiles):
    h, _, c = tiles.shape
    split = tiles.astype(f32).reshape(h, 2, HG, c)
    return [split[:, n].reshape(h * HG, c).astype(bf16) for n in range(2)]


def build_heads(diag, tiles):
    parts = [dot(diag, half) for half in halves(tiles)]
    k = diag.shape[0] // HG
    parts = [part.reshape(k, 1, HG, part.shape[1]) for part in parts]
    return jnp.concatenate(parts, axis=1).reshape(k, 2 * HG, parts[0].shape[3]).astype(bf16)


def spread_t(hidden):
    k, h = hidden.shape
    rows = lax.broadcasted_iota(i32, (h * DG, h), 0) // DG
    pick = (rows == lax.broadcasted_iota(i32, (h * DG, h), 1)).astype(bf16)
    tall = dot(pick, hidden, ((1,), (1,))).astype(bf16)
    columns = lax.broadcasted_iota(i32, (k, k * DG), 1) // DG
    widen = (columns == lax.broadcasted_iota(i32, (k, k * DG), 0)).astype(bf16)
    full = dot(tall, widen)
    d = lax.broadcasted_iota(i32, full.shape, 0) % DG
    same = d == lax.broadcasted_iota(i32, full.shape, 1) % DG
    return jnp.where(same, full, 0.0).astype(bf16)


def remote(src, dst, send, recv, dp, hyper):
    return pltpu.make_async_remote_copy(
        src_ref=src, dst_ref=dst, send_sem=send, recv_sem=recv, device_id={"dp": dp, "hyper": hyper}
    )


class Flood:
    def __init__(self, out, sems, n_dp, half):
        self.out, self.sems = out, sems
        self.na, self.half, self.n_hyper = n_dp // 2, half, 2 * half
        self.i, self.j, self.partner = place()
        self.a, self.b = self.i // 2, lax.rem(self.i, 2)
        self.cut = out.shape[2] // 32 * 16
        self.tall = out.shape[2]
        self.copies = {}

    @staticmethod
    def scratch(n_dp, half):
        dma, na = pltpu.SemaphoreType.DMA, n_dp // 2
        shapes = [(na,), (na,), (na, half), (na, half), (na, half), (na, 2, half)]
        return [dma(s) for s in shapes for _ in range(2)]

    def at(self, t, b, u):
        dp = source(self.a, t, self.na) * 2 + (self.b if b == 0 else 1 - self.b)
        return dp, lax.rem(self.j + self.n_hyper - 2 * u, self.n_hyper)

    def send(self, kind, index, block, where, dp, hyper, rows=None):
        number = "zxypqc".index(kind)
        s, r = self.sems[2 * number], self.sems[2 * number + 1]
        target = self.out.at[where[0], where[1]]
        if rows is not None:
            block, target = block.at[pl.ds(*rows)], target.at[pl.ds(*rows)]
        copy = remote(block, target, s.at[index], r.at[index], dp, hyper)
        copy.start()
        self.copies[kind, index] = copy

    def recv(self, kind, index):
        self.copies[kind, index].wait_recv()

    def peers(self):
        return [(u, lax.rem(self.j + 2 * u, self.n_hyper)) for u in range(1, self.half)]

    def column(self, t, own=None):
        where = self.at(t, 0, 0)
        if t:
            self.recv("z", (t,))
        block = self.out.at[where[0], where[1]] if own is None else own
        for u, peer in self.peers():
            self.send("y", (t, u), block, where, self.i, peer)
        self.send("x", (t,), block, where, self.a * 2 + 1 - self.b, self.j)
        self.send("c", (t, 0, 0), block, where, self.i, self.partner)

    def begin(self, own):
        where = self.at(0, 0, 0)
        for t in range(1, self.na):
            self.send("z", (t,), own, where, swap(self.a, t, self.na) * 2 + self.b, self.j)
        self.column(0, own)

    def pair(self, t):
        where = self.at(t, 1, 0)
        self.recv("x", (t,))
        block = self.out.at[where[0], where[1]]
        for u, peer in self.peers():
            self.send("p", (t, u), block, where, self.i, peer, (0, self.cut))
        self.send("c", (t, 1, 0), block, where, self.i, self.partner)

    def across(self, t):
        for u, peer in self.peers():
            where = self.at(t, 0, u)
            self.recv("y", (t, u))
            block = self.out.at[where[0], where[1]]
            self.send("c", (t, 0, u), block, where, self.i, self.partner)
            self.send(
                "q", (t, u), block, where, self.a * 2 + 1 - self.b, self.j, (self.cut, self.tall - self.cut)
            )

    def corner(self, t):
        for u, peer in self.peers():
            where = self.at(t, 1, u)
            self.recv("p", (t, u))
            self.recv("q", (t, u))
            self.send("c", (t, 1, u), self.out.at[where[0], where[1]], where, self.i, self.partner)

    def near(self, t):
        for u in range(self.half):
            self.recv("c", (t, 0, u))

    def far(self, t):
        for u in range(self.half):
            self.recv("c", (t, 1, u))

    def end(self):
        for copy in self.copies.values():
            copy.wait_send()


def hypernet(tiles, own, emb, hin_t, hb):
    blocks = tiles.shape[0]
    tiles = tiles.astype(f32)
    ids = (tiles[:, :8] * 256.0 + tiles[:, 8:]).reshape(blocks * 8, tiles.shape[2])[:, :1]
    clients = emb.shape[0]
    wide = (ids == lax.broadcasted_iota(i32, (blocks * 8, clients), 1).astype(f32)).astype(f32).astype(bf16)
    slots = blocks * own
    row = lax.broadcasted_iota(i32, (slots, blocks * 8), 0)
    column = lax.broadcasted_iota(i32, (slots, blocks * 8), 1)
    keep = (column == row // own * 8 + row % own).astype(f32).astype(bf16)
    select = dot(keep, wide).astype(bf16)
    picked = dot(select, emb).astype(bf16)
    preact = dot(picked, hin_t, ((1,), (1,))) + hb
    hidden = (preact / (1.0 + jnp.exp(-preact))).astype(bf16)
    return select, picked, preact, hidden


def main_kernel(
    n_dp, half, own, rows, aligned,
    x_ref, ids_ref, lab_ref, ew_ref, eb_ref, wn_ref, bn_ref, emb_ref, hin_ref, hb_ref, ho_ref,
    gw_all, dh_all, go_out, pre_out, picked_out, select_out,
    packed, xg, dl_all, own_dl, w_wide, w_narrow, bufs, ho_n, diag_f, heads_f, part,
    from_partner, summed, from_peer, diag, heads, dheads, diag_t, go, go_acc, feats, slopes, dpre,
    gw_acc, gb_acc, gw_own, dh_mine, b1, b2, dh_sum, hid_out, bias_w, id_own, id_all, local_sems, buf_sems,
    sp, rp, sq, rq, si, ri, sa, ra, sb, rb, sc, rc, *floods
):
    count = len(floods) // 3
    i, j, partner = place()
    n_hyper = 2 * half
    tall, width = x_ref.shape
    hh, wide, classes = ho_ref.shape
    chunk = bufs.shape[2]
    chunks = wide // chunk
    narrow = wide // n_dp
    groups = narrow // DG
    depth = bufs.shape[0]
    slots = n_dp * n_hyper * own
    group = n_hyper * own
    CS = diag.shape[0] // HG

    def buffer(c, slot):
        at = pl.ds(pl.multiple_of(c * chunk, chunk), chunk)
        return pltpu.make_async_copy(ho_ref.at[:, at, :], bufs.at[slot], buf_sems.at[slot])

    for c in range(min(depth, chunks)):
        buffer(c, c).start()
    wide_at = pl.ds(pl.multiple_of(j * wide, 128), wide)
    get_w = pltpu.make_async_copy(ew_ref.at[:, wide_at], w_wide, local_sems.at[0])
    get_w.start()
    get_h = pltpu.make_async_copy(
        ho_ref.at[:, pl.ds(pl.multiple_of(i * narrow, narrow), narrow), :], ho_n, local_sems.at[1]
    )
    get_h.start()
    first = (j * n_dp + i) * narrow
    if aligned:
        narrow_at = pl.ds(pl.multiple_of(first, 128), narrow)
        get_n = pltpu.make_async_copy(ew_ref.at[:, narrow_at], w_narrow, local_sems.at[2])
        get_n.start()

    row = lax.broadcasted_iota(i32, (16, width), 0)
    tile = jnp.zeros((16, width), f32)
    for s in range(own):
        number = ids_ref[s]
        tile = jnp.where(row == s, (number // 256).astype(f32), tile)
        tile = jnp.where(row == 8 + s, (number % 256).astype(f32), tile)
    packed[:tall] = x_ref[...]
    packed[tall:] = tile.astype(bf16)
    id_own[...] = tile.astype(bf16)
    id_all[j] = tile.astype(bf16)
    xg[i, j, :tall] = x_ref[...]
    xg[i, j, tall:] = tile.astype(bf16)

    sem = pltpu.get_barrier_semaphore()
    others = [(swap(i, t, n_dp), j) for t in range(1, n_dp)]
    others += [(i, lax.rem(j + u, n_hyper)) for u in range(1, n_hyper)]
    for dp, hyper in others:
        pl.semaphore_signal(sem, 1, device_id={"dp": dp, "hyper": hyper})
    pl.semaphore_wait(sem, len(others))

    na = n_dp // 2
    inp = Flood(xg, floods[:count], n_dp, half)
    to_ids = []
    for u in range(1, n_hyper):
        copy = remote(id_own, id_all.at[j], si.at[u], ri.at[u], i, lax.rem(j + u, n_hyper))
        copy.start()
        to_ids.append(copy)
    inp.begin(packed)
    for copy in to_ids:
        copy.wait_recv()
    small = (emb_ref[...], hin_ref[...], hb_ref[...])
    diag_f[...] = spread(hypernet(id_all[...], own, *small)[3])
    part[...] = jnp.zeros_like(part)
    bias_w[...] = eb_ref[pl.ds(pl.multiple_of(j * wide, 256), wide)].astype(f32)[None]
    get_w.wait()
    inp.across(0)
    inp.near(0)

    def forward(c, carry):
        slot = lax.rem(c, depth)
        buffer(c, slot).wait()
        for g in range(chunk // DG):
            spot = slice(g * DG, (g + 1) * DG)
            heads_f[:, spot, :] = build_heads(diag_f[...], bufs[slot, :, spot, :])

        @pl.when(c + depth < chunks)
        def _():
            buffer(c + depth, slot).start()

        w = w_wide[:, pl.ds(pl.multiple_of(c * chunk, chunk), chunk)]
        bias = bias_w[:, pl.ds(pl.multiple_of(c * chunk, chunk), chunk)]
        for p in range(n_hyper):
            pre = dot(xg[i, p, :tall, :], w) + bias
            feat = (pre / (1.0 + jnp.exp(-pre))).astype(bf16)
            for s in range(own):
                part[p, s * rows : (s + 1) * rows, :] += dot(feat[s * rows : (s + 1) * rows], heads_f[p * own + s])
        return carry

    lax.fori_loop(0, chunks // 2, forward, 0)
    for t in range(1, na):
        inp.column(t)
    inp.pair(0)
    lax.fori_loop(chunks // 2, chunks, forward, 0)
    for t in range(1, na):
        inp.pair(t)
        inp.across(t)
    inp.corner(0)

    to_partner = {}
    for u in list(range(1, half)) + [0]:
        to_partner[u] = remote(
            part.at[lax.rem(partner + 2 * u, n_hyper)], from_partner.at[u], sp.at[u], rp.at[u], i, partner
        )
        to_partner[u].start()
    to_peer = {}
    for u in range(1, half):
        peer = lax.rem(j + 2 * u, n_hyper)
        to_partner[u].wait_recv()
        summed[u] = part[peer] + from_partner[u]
        to_peer[u] = remote(summed.at[u], from_peer.at[u], sq.at[u], rq.at[u], i, peer)
        to_peer[u].start()
    for t in range(1, na):
        inp.corner(t)
        inp.near(t)
    for t in range(na):
        inp.far(t)
    tiles = xg[:, :, tall:, :].reshape(n_dp * n_hyper, 16, width)
    select, picked, preact, hidden = hypernet(tiles, own, *small)
    select_out[...] = select
    picked_out[...] = picked
    pre_out[...] = preact
    hid_out[...] = hidden
    if aligned:
        get_n.wait()
        bias_n = bias_w[:, pl.ds(pl.multiple_of(i * narrow, 128), narrow)]
        w_n = w_narrow
    else:
        bias_n = bn_ref[...].astype(f32)
        w_n = wn_ref

    nq = CS // group

    def prepare(base):
        mine = hid_out[pl.ds(pl.multiple_of(base * group, group), CS), :]
        diag[...] = spread(mine)

        def features(q, carry):
            for p in range(n_hyper):
                pre = dot(xg[base + q, p, :tall, :], w_n[...]) + bias_n
                logistic = 1.0 / (1.0 + jnp.exp(-pre))
                at = pl.ds(pl.multiple_of((q * n_hyper + p) * tall, tall), tall)
                feats[at, :] = (pre * logistic).astype(bf16)
                slopes[at, :] = logistic * (1.0 + pre * (1.0 - logistic))
            return carry

        lax.fori_loop(0, nq, features, 0)

    single = nq == n_dp
    if single:
        prepare(0)
        diag_t[...] = spread_t(hidden)
    to_partner[0].wait_recv()
    logits = part[j] + from_partner[0]
    for u in range(1, half):
        to_peer[u].wait_recv()
        logits = logits + from_peer[u]
    eye = lax.broadcasted_iota(i32, (rows, rows), 0) == lax.broadcasted_iota(i32, (rows, rows), 1)
    columns = []
    for s in range(own):
        spot = jnp.where(eye, lab_ref[s : s + 1, :], 0)
        columns.append(jnp.sum(spot, axis=1, keepdims=True))
    label = jnp.concatenate(columns, axis=0)
    largest = jnp.max(logits, axis=-1, keepdims=True)
    exponent = jnp.exp(logits - largest)
    probability = exponent / jnp.sum(exponent, axis=-1, keepdims=True)
    onehot = (label == lax.broadcasted_iota(i32, logits.shape, 1)).astype(f32)
    dl = ((probability - onehot) / rows).astype(bf16)
    own_dl[...] = dl
    dl_all[i, j] = dl
    grads = Flood(dl_all, floods[count : 2 * count], n_dp, half)
    grads.begin(own_dl)

    gw_acc[...] = jnp.zeros_like(gw_acc)
    gb_acc[...] = jnp.zeros_like(gb_acc)

    def ho_group(g):
        return ho_n[:, pl.ds(pl.multiple_of(g * DG, DG), DG), :].reshape(hh * DG, classes)

    def heads_part(low, high):
        def step(g, carry):
            at = pl.ds(pl.multiple_of(g * DG, DG), DG)
            heads[:, at, :] = build_heads(diag[...], ho_n[:, at, :])
            return carry

        lax.fori_loop(low, high, step, 0)

    def slots_part(base, low):
        def step(n, carry):
            q = low + n
            gw, gb = gw_acc[...], gb_acc[...]
            for p in range(n_hyper):
                block = (q - base) * n_hyper + p
                for s in range(own):
                    dl_s = dl_all[q, p, s * rows : (s + 1) * rows, :]
                    at = pl.ds(pl.multiple_of(block * tall + s * rows, rows), rows)
                    slot = (q * n_hyper + p) * own + s
                    dhead = dot(feats[at, :], dl_s, ((0,), (0,))).astype(bf16)
                    dheads[:, pl.ds(pl.multiple_of(slot * DG, DG), DG), :] = dhead.reshape(groups, DG, classes)
                    dfeat = dot(dl_s, heads[block * own + s], ((1,), (1,))).astype(bf16)
                    dpre[at, :] = (dfeat.astype(f32) * slopes[at, :]).astype(bf16)
            for p in range(n_hyper):
                block = (q - base) * n_hyper + p
                both = dpre[pl.ds(pl.multiple_of(block * tall, tall), tall), :]
                gw = gw + dot(xg[q, p, :tall, :], both, ((0,), (0,)))
                gb = gb + jnp.sum(both.astype(f32), axis=0, keepdims=True)
            gw_acc[...], gb_acc[...] = gw, gb
            return carry

        lax.fori_loop(0, 2, step, 0)

    def go_part(low, high):
        def step(g, carry):
            at = pl.ds(pl.multiple_of(g * DG, DG), DG)
            go[:, at, :] = dot(diag_t[...], dheads[g]).astype(bf16).reshape(hh, DG, classes)
            return carry

        if single:
            lax.fori_loop(low, high, step, 0)

    def total_part(q0):
        count = 2 * group * DG
        at = pl.ds(pl.multiple_of(q0 * group * DG, group * DG), count)
        z = dot(ho_group(0), dheads[0, at, :], ((1,), (1,)))
        for g in range(1, groups):
            z = z + dot(ho_group(g), dheads[g, at, :], ((1,), (1,)))
        d = lax.broadcasted_iota(i32, z.shape, 0) % DG
        same = d == lax.broadcasted_iota(i32, z.shape, 1) % DG
        kept = jnp.sum(jnp.where(same, z, 0.0).reshape(hh, DG, count), axis=1)
        kept = jnp.concatenate([kept, jnp.zeros((128 - hh, count), f32)], axis=0)
        fold = lax.broadcasted_iota(i32, (2 * group, count), 1) // DG
        fold = (fold == lax.broadcasted_iota(i32, (2 * group, count), 0)).astype(f32)
        mine = dot(fold, kept, ((1,), (1,)), precision=highest)
        dh_mine[pl.ds(pl.multiple_of(q0 * group, group), 2 * group), :] = mine

    def flood_first(flood, work, count):
        cuts = [count * (t + 1) // na for t in range(na)]
        done = 0
        for t in range(1, na):
            work(done, cuts[t - 1])
            done = cuts[t - 1]
            flood.column(t)
            flood.pair(t - 1)
            flood.across(t - 1)
        flood.corner(0)
        work(done, count)
        flood.pair(na - 1)
        flood.across(na - 1)

    get_h.wait()
    if single:
        flood_first(grads, heads_part, groups)
        for t in range(na):
            if t + 1 < na:
                grads.corner(t + 1)
            grads.near(t)
            grads.far(t)
            slots_part(0, source(grads.a, t, na) * 2)
            if t + 1 < na:
                total_part(source(grads.a, t, na) * 2)
    else:
        flood_first(grads, lambda low, high: None, groups)
        for t in range(na):
            if t + 1 < na:
                grads.corner(t + 1)
            grads.near(t)
            grads.far(t)

        def one(q, carry):
            prepare(q * nq)
            heads_part(0, groups)
            for n in range(nq // 2):
                slots_part(q * nq, q * nq + 2 * n)
            for n in range(nq // 2):
                total_part(q * nq + 2 * n)
            diag_t[...] = spread_t(hid_out[pl.ds(pl.multiple_of(q * CS, CS), CS), :])
            at = pl.ds(pl.multiple_of(q * CS * DG, CS * DG), CS * DG)
            for g in range(groups):
                spot = slice(g * DG, (g + 1) * DG)
                go_acc[:, spot, :] += dot(diag_t[...], dheads[g, at, :]).reshape(hh, DG, classes)
            return carry

        go_acc[...] = jnp.zeros_like(go_acc)

        lax.fori_loop(0, n_dp // nq, one, 0)
        go[...] = go_acc[...].astype(bf16)
    gw_own[:width] = gw_acc[...].astype(bf16)
    gw_own[width:] = jnp.broadcast_to(gb_acc[...], (16, narrow)).astype(bf16)
    if aligned:
        gw_all[i, j] = gw_own[...]
    else:
        put_own = pltpu.make_async_copy(gw_own, gw_all.at[i, j], local_sems.at[2])
        put_own.start()
        put_own.wait()
    fin = Flood(gw_all, floods[2 * count :], n_dp, half)
    fin.begin(gw_own)
    if single:
        total_part(source(grads.a, na - 1, na) * 2)

    share = slots // n_hyper
    peers = [lax.rem(j + u, n_hyper) for u in range(1, n_hyper)]
    to_hyper = []
    for u in range(1, n_hyper):
        at = pl.ds(pl.multiple_of(peers[u - 1] * share, share), share)
        copy = remote(dh_mine.at[at], b1.at[u], sa.at[u], ra.at[u], i, peers[u - 1])
        copy.start()
        to_hyper.append(copy)
    quart = groups // 4
    go_part(0, quart)
    fin.column(1)
    fin.pair(0)
    fin.across(0)
    quarter = dh_mine[pl.ds(pl.multiple_of(j * share, share), share), :]
    for u in range(1, n_hyper):
        to_hyper[u - 1].wait_recv()
        quarter = quarter + b1[u]
    dh_sum[0] = quarter
    b2[i] = quarter
    to_dp = []
    for t in range(1, n_dp):
        copy = remote(dh_sum.at[0], b2.at[i], sb.at[t], rb.at[t], swap(i, t, n_dp), j)
        copy.start()
        to_dp.append(copy)
    go_part(quart, 2 * quart)
    for t in range(2, na):
        fin.column(t)
        fin.pair(t - 1)
        fin.across(t - 1)
    fin.corner(0)
    go_part(2 * quart, 3 * quart)
    for copy in to_dp:
        copy.wait_recv()
    sum_all = b2[0]
    for t in range(1, n_dp):
        sum_all = sum_all + b2[t]
    dh_sum[1] = sum_all
    dh_all[j] = sum_all
    last = []
    for u in range(1, n_hyper):
        copy = remote(dh_sum.at[1], dh_all.at[j], sc.at[u], rc.at[u], i, peers[u - 1])
        copy.start()
        last.append(copy)
    fin.pair(na - 1)
    fin.across(na - 1)
    go_part(3 * quart, groups)
    put_go = pltpu.make_async_copy(go, go_out, local_sems.at[3])
    put_go.start()
    for t in range(1, na):
        fin.corner(t)
    for t in range(na):
        fin.near(t)
        fin.far(t)
    for copy in last:
        copy.wait_recv()
    put_go.wait()
    for copy in list(to_partner.values()) + list(to_peer.values()) + to_hyper + to_dp + last + to_ids:
        copy.wait_send()
    for flood in (inp, grads, fin):
        flood.end()


def main_part(x, ids, labels, ew, eb, wn, bn, emb, hin_t, hb, ho, n_dp, n_hyper, aligned):
    own, rows = labels.shape
    tall, width = x.shape
    hh, wide, classes = ho.shape
    narrow = wide // n_dp
    half = n_hyper // 2
    group = n_hyper * own
    slots = group * n_dp
    CS = slots if slots <= 64 else 2 * group
    chunk = 128
    depth = 3 if slots <= 64 else 2
    block = tall + 16
    share = slots // n_hyper
    dma = pltpu.SemaphoreType.DMA
    sample = CS * rows
    vm = pltpu.VMEM
    ANY = pl.BlockSpec(memory_space=pl.ANY)
    shape = jax.ShapeDtypeStruct
    return pl.pallas_call(
        functools.partial(main_kernel, n_dp, half, own, rows, aligned),
        out_shape=(
            shape((n_dp, n_hyper, width + 16, narrow), bf16),
            shape((n_hyper, share, 128), f32),
            shape((hh, narrow, classes), bf16),
            shape((slots, hh), f32),
            shape((slots, emb.shape[1]), bf16),
            shape((slots, emb.shape[0]), bf16),
        ),
        in_specs=[VM, pl.BlockSpec(memory_space=pltpu.SMEM), VM, ANY, VM, VM, VM, VM, VM, VM, ANY],
        out_specs=(VM if aligned else ANY, VM, ANY, VM, VM, VM),
        scratch_shapes=[
            vm((block, width), bf16),
            vm((n_dp, n_hyper, block, width), bf16),
            vm((n_dp, n_hyper, tall, classes), bf16),
            vm((tall, classes), bf16),
            vm((width, wide), bf16),
            vm((width, narrow), bf16),
            vm((depth, hh, chunk, classes), bf16),
            vm((hh, narrow, classes), bf16),
            vm((group * HG, hh * HG), bf16),
            vm((group, chunk, classes), bf16),
            vm((n_hyper, tall, classes), f32),
            vm((half, tall, classes), f32),
            vm((half, tall, classes), f32),
            vm((half, tall, classes), f32),
            vm((CS * HG, hh * HG), bf16),
            vm((CS, narrow, classes), bf16),
            vm((narrow // DG, slots * DG, classes), bf16),
            vm((hh * DG, CS * DG), bf16),
            vm((hh, narrow, classes), bf16),
            vm((8, 8, 128) if CS == slots else (hh, narrow, classes), f32),
            vm((sample, narrow), bf16),
            vm((sample, narrow), f32),
            vm((sample, narrow), bf16),
            vm((width, narrow), f32),
            vm((1, narrow), f32),
            vm((width + 16, narrow), bf16),
            vm((slots, 128), f32),
            vm((n_hyper, share, 128), f32),
            vm((n_dp, share, 128), f32),
            vm((2, share, 128), f32),
            vm((slots, hh), bf16),
            vm((1, wide), f32),
            vm((16, width), bf16),
            vm((n_hyper, 16, width), bf16),
            dma((4,)),
            dma((depth,)),
        ]
        + [dma((half,)) for _ in range(4)]
        + [dma((n_hyper,)), dma((n_hyper,))]
        + [dma((n_hyper,)), dma((n_hyper,)), dma((n_dp,)), dma((n_dp,)), dma((n_hyper,)), dma((n_hyper,))]
        + Flood.scratch(n_dp, half) * 3,
        compiler_params=pltpu.CompilerParams(
            collective_id=0, has_side_effects=True, vmem_limit_bytes=LIMIT
        ),
        name="main_part",
    )(x, ids, labels, ew, eb, wn, bn, emb, hin_t, hb, ho)


def last_kernel(aligned, pieces, go_in, gw_in, pre_ref, picked_ref, select_ref, hin_ref, dh_ref,
                go_out, gwf_out, gb_ref, table_ref, in_ref, hb_ref, go_b, go_f, gw_ref, gwf_ref, sems):
    hh, wide, _ = go_b.shape
    per = wide // pieces
    reads, writes = [], []
    for n in range(pieces):
        at = slice(n * per, (n + 1) * per)
        reads.append(pltpu.make_async_copy(go_in.at[:, at, :], go_b.at[:, at, :], sems.at[0, n]))
        writes.append(pltpu.make_async_copy(go_f.at[:, at, :], go_out.at[:, at, :], sems.at[1, n]))
        reads[n].start()
    get = pltpu.make_async_copy(gw_in, gw_ref, sems.at[2, 0])
    put = pltpu.make_async_copy(gwf_ref, gwf_out, sems.at[2, 1])
    if aligned:
        get.start()
    for n in range(pieces):
        at = slice(n * per, (n + 1) * per)
        reads[n].wait()
        go_f[:, at, :] = go_b[:, at, :].astype(f32)
        writes[n].start()
    if aligned:
        get.wait()
        n_dp, n_hyper, tall, narrow = gw_ref.shape
        for jj in range(n_hyper):
            for ii in range(n_dp):
                at = (jj * n_dp + ii) * narrow
                gwf_ref[:, at : at + narrow] = gw_ref[ii, jj, : tall - 16, :].astype(f32)
                gb_ref[:, at : at + narrow] = gw_ref[ii, jj, tall - 16 : tall - 8, :].astype(f32)[:1]
        put.start()
    dpre = dh_ref[...][:, :hh] * silu_slope(pre_ref[...])
    hb_ref[...] = jnp.sum(dpre, axis=0, keepdims=True)
    in_ref[...] = dot(dpre, picked_ref[...].astype(f32), ((0,), (0,)), precision=highest)
    back = dot(dpre, hin_ref[...].astype(f32), precision=highest)
    table_ref[...] = dot(select_ref[...].astype(f32), back, ((0,), (0,)), precision=highest)
    for copy in writes:
        copy.wait()
    if aligned:
        put.wait()


def last_part(go, pre, picked, select, hin_t, dh, gw_all, aligned):
    hh, wide, classes = go.shape
    width = picked.shape[1]
    clients = select.shape[1]
    n_dp, n_hyper, block, narrow = gw_all.shape
    shape = jax.ShapeDtypeStruct
    full = (block - 16, n_dp * n_hyper * narrow) if aligned else (8, 128)
    given = gw_all if aligned else gw_all[:1, :1]
    pieces = 4 if wide % 64 == 0 else 1
    ANY = pl.BlockSpec(memory_space=pl.ANY)
    return pl.pallas_call(
        functools.partial(last_kernel, aligned, pieces),
        out_shape=(
            shape(go.shape, f32),
            shape(full, f32),
            shape((1, full[1]), f32),
            shape((clients, hin_t.shape[1]), f32),
            shape((hh, width), f32),
            shape((1, hh), f32),
        ),
        in_specs=[ANY, ANY, VM, VM, VM, VM, VM],
        out_specs=(ANY, ANY, VM, VM, VM, VM),
        scratch_shapes=[
            pltpu.VMEM(go.shape, bf16),
            pltpu.VMEM(go.shape, f32),
            pltpu.VMEM(given.shape, bf16),
            pltpu.VMEM(full, f32),
            pltpu.SemaphoreType.DMA((3, 4)),
        ],
        compiler_params=pltpu.CompilerParams(vmem_limit_bytes=LIMIT),
        name="last_part",
    )(go, given, pre, picked, select, hin_t, dh)


def local(
    inputs, labels, client_ids, ext_weight, ext_bias, embeddings, hyper_in, hyper_bias, hyper_out
):
    n_dp, n_hyper = lax.axis_size("dp"), lax.axis_size("hyper")
    own, rows, width = inputs.shape
    narrow = hyper_out.shape[0] // n_dp
    aligned = narrow % 128 == 0
    ho = hyper_out.transpose(1, 0, 2)
    hin_t = hyper_in.T
    bias = ext_bias
    if aligned:
        wn, bn = embeddings, hyper_bias[None]
    else:
        start = (lax.axis_index("hyper") * n_dp + lax.axis_index("dp")) * narrow
        wn = lax.dynamic_slice_in_dim(ext_weight, start, narrow, 1)
        bn = lax.dynamic_slice_in_dim(bias, start, narrow, 0)[None]
    gw_all, dh, go, pre, picked, select = main_part(
        inputs.reshape(own * rows, width), client_ids, labels, ext_weight, bias, wn, bn,
        embeddings, hin_t, hyper_bias[None], ho, n_dp, n_hyper, aligned,
    )
    grad_out, gw, gb, table, grad_in, grad_hb = last_part(
        go, pre, picked, select, hin_t, dh.reshape(-1, 128), gw_all, aligned
    )
    if not aligned:
        gw = gw_all[:, :, :width].transpose(2, 1, 0, 3).reshape(width, -1).astype(f32)
        gb = gw_all[:, :, width].transpose(1, 0, 2).reshape(-1).astype(f32)
    return (gw, gb.reshape(-1), table, grad_in.T, grad_hb.reshape(-1), grad_out.transpose(1, 0, 2))


def solution(mesh):
    placed = (
        P(("dp", "hyper"), None, None),
        P(("dp", "hyper"), None),
        P(("dp", "hyper")),
        P(),
        P(),
        P(),
        P(),
        P(),
        P("hyper", None, None),
    )
    return jax.shard_map(
        local,
        mesh=mesh,
        in_specs=placed,
        out_specs=(P(), P(), P(), P(), P(), P(("hyper", "dp"), None, None)),
        check_vma=False,
    )
```

```python
import functools

import jax
import jax.numpy as jnp
from jax import lax
from jax.experimental import pallas as pl
from jax.experimental.pallas import tpu as pltpu
from jax.sharding import PartitionSpec as P

highest = lax.Precision.HIGHEST
f32 = jnp.float32
bf16 = jnp.bfloat16
i32 = jnp.int32
VM = pl.BlockSpec(memory_space=pltpu.VMEM)
DG = 16
HG = 8
LIMIT = 60 * 1024 * 1024


def silu_slope(values):
    logistic = jax.nn.sigmoid(values)
    return logistic * (1.0 + values * (1.0 - logistic))


def dot(a, b, dims=((1,), (0,)), **kw):
    return lax.dot_general(a, b, (dims, ((), ())), preferred_element_type=f32, **kw)


def swap(index, other, count):
    if count & (count - 1):
        return lax.rem(index + other, count)
    out = index
    bit = 1
    while bit < count:
        if other & bit:
            out = out + bit - 2 * bit * lax.rem(index // bit, 2)
        bit *= 2
    return out


def source(index, other, count):
    if count & (count - 1):
        return lax.rem(index + count - other, count)
    return swap(index, other, count)


def place():
    i, j = lax.axis_index("dp"), lax.axis_index("hyper")
    return i, j, j + 1 - 2 * lax.rem(j, 2)


def spread(hidden, slots=0, own=0):
    k, h = hidden.shape
    slots = slots or k
    rows = lax.broadcasted_iota(i32, (slots * HG, k), 0) // HG
    if own:
        rows = rows // own * 16 + rows % own
    pick = (rows == lax.broadcasted_iota(i32, (slots * HG, k), 1)).astype(bf16)
    tall = dot(pick, hidden).astype(bf16)
    columns = lax.broadcasted_iota(i32, (h, h * HG), 1) // HG
    widen = (columns == lax.broadcasted_iota(i32, (h, h * HG), 0)).astype(bf16)
    full = dot(tall, widen)
    d = lax.broadcasted_iota(i32, full.shape, 0) % HG
    same = d == lax.broadcasted_iota(i32, full.shape, 1) % HG
    return jnp.where(same, full, 0.0).astype(bf16)


def halves(tiles):
    h, _, c = tiles.shape
    split = tiles.astype(f32).reshape(h, 2, HG, c)
    return [split[:, n].reshape(h * HG, c).astype(bf16) for n in range(2)]


def build_heads(diag, tiles):
    parts = [dot(diag, half) for half in halves(tiles)]
    k = diag.shape[0] // HG
    parts = [part.reshape(k, 1, HG, part.shape[1]) for part in parts]
    return jnp.concatenate(parts, axis=1).reshape(k, 2 * HG, parts[0].shape[3]).astype(bf16)


def spread_t(hidden):
    k, h = hidden.shape
    rows = lax.broadcasted_iota(i32, (h * DG, h), 0) // DG
    pick = (rows == lax.broadcasted_iota(i32, (h * DG, h), 1)).astype(bf16)
    tall = dot(pick, hidden, ((1,), (1,))).astype(bf16)
    columns = lax.broadcasted_iota(i32, (k, k * DG), 1) // DG
    widen = (columns == lax.broadcasted_iota(i32, (k, k * DG), 0)).astype(bf16)
    full = dot(tall, widen)
    d = lax.broadcasted_iota(i32, full.shape, 0) % DG
    same = d == lax.broadcasted_iota(i32, full.shape, 1) % DG
    return jnp.where(same, full, 0.0).astype(bf16)


def remote(src, dst, send, recv, dp, hyper):
    return pltpu.make_async_remote_copy(
        src_ref=src, dst_ref=dst, send_sem=send, recv_sem=recv, device_id={"dp": dp, "hyper": hyper}
    )


class Flood:
    def __init__(self, out, sems, n_dp, half):
        self.out, self.sems = out, sems
        self.na, self.half, self.n_hyper = n_dp // 2, half, 2 * half
        self.i, self.j, self.partner = place()
        self.a, self.b = self.i // 2, lax.rem(self.i, 2)
        self.cut = out.shape[2] // 32 * 16
        self.tall = out.shape[2]
        self.copies = {}

    @staticmethod
    def scratch(n_dp, half):
        dma, na = pltpu.SemaphoreType.DMA, n_dp // 2
        shapes = [(na,), (na,), (na, half), (na, half), (na, half), (na, 2, half)]
        return [dma(s) for s in shapes for _ in range(2)]

    def at(self, t, b, u):
        dp = source(self.a, t, self.na) * 2 + (self.b if b == 0 else 1 - self.b)
        return dp, lax.rem(self.j + self.n_hyper - 2 * u, self.n_hyper)

    def send(self, kind, index, block, where, dp, hyper, rows=None):
        number = "zxypqc".index(kind)
        s, r = self.sems[2 * number], self.sems[2 * number + 1]
        target = self.out.at[where[0], where[1]]
        if rows is not None:
            block, target = block.at[pl.ds(*rows)], target.at[pl.ds(*rows)]
        copy = remote(block, target, s.at[index], r.at[index], dp, hyper)
        copy.start()
        self.copies[kind, index] = copy

    def recv(self, kind, index):
        self.copies[kind, index].wait_recv()

    def peers(self):
        return [(u, lax.rem(self.j + 2 * u, self.n_hyper)) for u in range(1, self.half)]

    def column(self, t, own=None):
        where = self.at(t, 0, 0)
        if t:
            self.recv("z", (t,))
        block = self.out.at[where[0], where[1]] if own is None else own
        for u, peer in self.peers():
            self.send("y", (t, u), block, where, self.i, peer)
        self.send("x", (t,), block, where, self.a * 2 + 1 - self.b, self.j)
        self.send("c", (t, 0, 0), block, where, self.i, self.partner)

    def begin(self, own):
        where = self.at(0, 0, 0)
        for t in range(1, self.na):
            self.send("z", (t,), own, where, swap(self.a, t, self.na) * 2 + self.b, self.j)
        self.column(0, own)

    def pair(self, t):
        where = self.at(t, 1, 0)
        self.recv("x", (t,))
        block = self.out.at[where[0], where[1]]
        for u, peer in self.peers():
            self.send("p", (t, u), block, where, self.i, peer, (0, self.cut))
        self.send("c", (t, 1, 0), block, where, self.i, self.partner)

    def across(self, t):
        for u, peer in self.peers():
            where = self.at(t, 0, u)
            self.recv("y", (t, u))
            block = self.out.at[where[0], where[1]]
            self.send("c", (t, 0, u), block, where, self.i, self.partner)
            self.send(
                "q", (t, u), block, where, self.a * 2 + 1 - self.b, self.j, (self.cut, self.tall - self.cut)
            )

    def corner(self, t):
        for u, peer in self.peers():
            where = self.at(t, 1, u)
            self.recv("p", (t, u))
            self.recv("q", (t, u))
            self.send("c", (t, 1, u), self.out.at[where[0], where[1]], where, self.i, self.partner)

    def near(self, t):
        for u in range(self.half):
            self.recv("c", (t, 0, u))

    def far(self, t):
        for u in range(self.half):
            self.recv("c", (t, 1, u))

    def end(self):
        for copy in self.copies.values():
            copy.wait_send()


def hypernet(tiles, own, emb, hin_t, hb):
    blocks = tiles.shape[0]
    tiles = tiles.astype(f32)
    ids = (tiles[:, :8] * 256.0 + tiles[:, 8:]).reshape(blocks * 8, tiles.shape[2])[:, :1]
    clients = emb.shape[0]
    wide = (ids == lax.broadcasted_iota(i32, (blocks * 8, clients), 1).astype(f32)).astype(f32).astype(bf16)
    slots = blocks * own
    row = lax.broadcasted_iota(i32, (slots, blocks * 8), 0)
    column = lax.broadcasted_iota(i32, (slots, blocks * 8), 1)
    keep = (column == row // own * 8 + row % own).astype(f32).astype(bf16)
    select = dot(keep, wide).astype(bf16)
    picked = dot(select, emb).astype(bf16)
    preact = dot(picked, hin_t, ((1,), (1,))) + hb
    hidden = (preact / (1.0 + jnp.exp(-preact))).astype(bf16)
    return select, picked, preact, hidden


def main_kernel(
    n_dp, half, own, rows, aligned,
    x_ref, ids_ref, lab_ref, ew_ref, eb_ref, wn_ref, bn_ref, emb_ref, hin_ref, hb_ref, ho_ref,
    gw_all, dh_all, go_out, pre_out, picked_out, select_out,
    packed, xg, dl_all, own_dl, w_wide, w_narrow, bufs, ho_n, diag_f, heads_f, part,
    from_partner, summed, from_peer, diag, heads, dheads, diag_t, go, go_acc, feats, slopes, dpre,
    gw_acc, gb_acc, gw_own, dh_mine, b1, b2, dh_sum, hid_out, bias_w, id_own, id_all, local_sems, buf_sems,
    sp, rp, sq, rq, si, ri, sa, ra, sb, rb, sc, rc, *floods
):
    count = len(floods) // 3
    i, j, partner = place()
    n_hyper = 2 * half
    tall, width = x_ref.shape
    hh, wide, classes = ho_ref.shape
    chunk = bufs.shape[2]
    chunks = wide // chunk
    narrow = wide // n_dp
    groups = narrow // DG
    depth = bufs.shape[0]
    slots = n_dp * n_hyper * own
    group = n_hyper * own
    CS = diag.shape[0] // HG

    def buffer(c, slot):
        at = pl.ds(pl.multiple_of(c * chunk, chunk), chunk)
        return pltpu.make_async_copy(ho_ref.at[:, at, :], bufs.at[slot], buf_sems.at[slot])

    for c in range(min(depth, chunks)):
        buffer(c, c).start()
    wide_at = pl.ds(pl.multiple_of(j * wide, 128), wide)
    get_w = pltpu.make_async_copy(ew_ref.at[:, wide_at], w_wide, local_sems.at[0])
    get_w.start()
    get_h = pltpu.make_async_copy(
        ho_ref.at[:, pl.ds(pl.multiple_of(i * narrow, narrow), narrow), :], ho_n, local_sems.at[1]
    )
    get_h.start()
    first = (j * n_dp + i) * narrow
    if aligned:
        narrow_at = pl.ds(pl.multiple_of(first, 128), narrow)
        get_n = pltpu.make_async_copy(ew_ref.at[:, narrow_at], w_narrow, local_sems.at[2])
        get_n.start()

    row = lax.broadcasted_iota(i32, (16, width), 0)
    tile = jnp.zeros((16, width), f32)
    for s in range(own):
        number = ids_ref[s]
        tile = jnp.where(row == s, (number // 256).astype(f32), tile)
        tile = jnp.where(row == 8 + s, (number % 256).astype(f32), tile)
    sem = pltpu.get_barrier_semaphore()
    others = [(swap(i, t, n_dp), j) for t in range(1, n_dp)]
    others += [(i, lax.rem(j + u, n_hyper)) for u in range(1, n_hyper)]
    for dp, hyper in others:
        pl.semaphore_signal(sem, 1, device_id={"dp": dp, "hyper": hyper})
    packed[:tall] = x_ref[...]
    packed[tall:] = tile.astype(bf16)
    small = (emb_ref[...], hin_ref[...], hb_ref[...])
    id_own[...] = jnp.zeros_like(id_own)
    id_own[:own, :hh] = hypernet(tile.astype(bf16)[None], own, *small)[3]
    id_all[j] = id_own[...]
    xg[i, j, :tall] = x_ref[...]
    xg[i, j, tall:] = tile.astype(bf16)
    pl.semaphore_wait(sem, len(others))

    na = n_dp // 2
    inp = Flood(xg, floods[:count], n_dp, half)
    to_ids = []
    for u in range(1, n_hyper):
        copy = remote(id_own, id_all.at[j], si.at[u], ri.at[u], i, lax.rem(j + u, n_hyper))
        copy.start()
        to_ids.append(copy)
    inp.begin(packed)
    for copy in to_ids:
        copy.wait_recv()
    diag_f[...] = spread(id_all[...].reshape(n_hyper * 16, width)[:, :hh], group, own)
    part[...] = jnp.zeros_like(part)
    bias_w[...] = eb_ref[pl.ds(pl.multiple_of(j * wide, 256), wide)].astype(f32)[None]
    get_w.wait()
    inp.across(0)
    inp.near(0)

    def forward(c, carry):
        slot = lax.rem(c, depth)
        buffer(c, slot).wait()
        for g in range(chunk // DG):
            spot = slice(g * DG, (g + 1) * DG)
            heads_f[:, spot, :] = build_heads(diag_f[...], bufs[slot, :, spot, :])

        @pl.when(c + depth < chunks)
        def _():
            buffer(c + depth, slot).start()

        w = w_wide[:, pl.ds(pl.multiple_of(c * chunk, chunk), chunk)]
        bias = bias_w[:, pl.ds(pl.multiple_of(c * chunk, chunk), chunk)]
        for p in range(n_hyper):
            pre = dot(xg[i, p, :tall, :], w) + bias
            feat = (pre / (1.0 + jnp.exp(-pre))).astype(bf16)
            for s in range(own):
                part[p, s * rows : (s + 1) * rows, :] += dot(feat[s * rows : (s + 1) * rows], heads_f[p * own + s])
        return carry

    lax.fori_loop(0, chunks // 2, forward, 0)
    for t in range(1, na):
        inp.column(t)
    inp.pair(0)
    lax.fori_loop(chunks // 2, chunks, forward, 0)
    for t in range(1, na):
        inp.pair(t)
        inp.across(t)
    inp.corner(0)

    to_partner = {}
    for u in list(range(1, half)) + [0]:
        to_partner[u] = remote(
            part.at[lax.rem(partner + 2 * u, n_hyper)], from_partner.at[u], sp.at[u], rp.at[u], i, partner
        )
        to_partner[u].start()
    to_peer = {}
    for u in range(1, half):
        peer = lax.rem(j + 2 * u, n_hyper)
        to_partner[u].wait_recv()
        summed[u] = part[peer] + from_partner[u]
        to_peer[u] = remote(summed.at[u], from_peer.at[u], sq.at[u], rq.at[u], i, peer)
        to_peer[u].start()
    for t in range(1, na):
        inp.corner(t)
        inp.near(t)
    for t in range(na):
        inp.far(t)
    tiles = xg[:, :, tall:, :].reshape(n_dp * n_hyper, 16, width)
    select, picked, preact, hidden = hypernet(tiles, own, *small)
    select_out[...] = select
    picked_out[...] = picked
    pre_out[...] = preact
    hid_out[...] = hidden
    if aligned:
        get_n.wait()
        bias_n = bias_w[:, pl.ds(pl.multiple_of(i * narrow, 128), narrow)]
        w_n = w_narrow
    else:
        bias_n = bn_ref[...].astype(f32)
        w_n = wn_ref

    nq = CS // group

    def prepare(base):
        mine = hid_out[pl.ds(pl.multiple_of(base * group, group), CS), :]
        diag[...] = spread(mine)

        def features(q, carry):
            for p in range(n_hyper):
                pre = dot(xg[base + q, p, :tall, :], w_n[...]) + bias_n
                logistic = 1.0 / (1.0 + jnp.exp(-pre))
                at = pl.ds(pl.multiple_of((q * n_hyper + p) * tall, tall), tall)
                feats[at, :] = (pre * logistic).astype(bf16)
                slopes[at, :] = logistic * (1.0 + pre * (1.0 - logistic))
            return carry

        lax.fori_loop(0, nq, features, 0)

    single = nq == n_dp
    if single:
        prepare(0)
        diag_t[...] = spread_t(hidden)
    to_partner[0].wait_recv()
    logits = part[j] + from_partner[0]
    for u in range(1, half):
        to_peer[u].wait_recv()
        logits = logits + from_peer[u]
    eye = lax.broadcasted_iota(i32, (rows, rows), 0) == lax.broadcasted_iota(i32, (rows, rows), 1)
    columns = []
    for s in range(own):
        spot = jnp.where(eye, lab_ref[s : s + 1, :], 0)
        columns.append(jnp.sum(spot, axis=1, keepdims=True))
    label = jnp.concatenate(columns, axis=0)
    largest = jnp.max(logits, axis=-1, keepdims=True)
    exponent = jnp.exp(logits - largest)
    probability = exponent / jnp.sum(exponent, axis=-1, keepdims=True)
    onehot = (label == lax.broadcasted_iota(i32, logits.shape, 1)).astype(f32)
    dl = ((probability - onehot) / rows).astype(bf16)
    own_dl[...] = dl
    dl_all[i, j] = dl
    grads = Flood(dl_all, floods[count : 2 * count], n_dp, half)
    grads.begin(own_dl)

    gw_acc[...] = jnp.zeros_like(gw_acc)
    gb_acc[...] = jnp.zeros_like(gb_acc)

    def ho_group(g):
        return ho_n[:, pl.ds(pl.multiple_of(g * DG, DG), DG), :].reshape(hh * DG, classes)

    def heads_part(low, high):
        def step(g, carry):
            at = pl.ds(pl.multiple_of(g * DG, DG), DG)
            heads[:, at, :] = build_heads(diag[...], ho_n[:, at, :])
            return carry

        lax.fori_loop(low, high, step, 0)

    def slots_part(base, low):
        def step(n, carry):
            q = low + n
            gw, gb = gw_acc[...], gb_acc[...]
            for p in range(n_hyper):
                block = (q - base) * n_hyper + p
                for s in range(own):
                    dl_s = dl_all[q, p, s * rows : (s + 1) * rows, :]
                    at = pl.ds(pl.multiple_of(block * tall + s * rows, rows), rows)
                    slot = (q * n_hyper + p) * own + s
                    dhead = dot(feats[at, :], dl_s, ((0,), (0,))).astype(bf16)
                    dheads[:, pl.ds(pl.multiple_of(slot * DG, DG), DG), :] = dhead.reshape(groups, DG, classes)
                    dfeat = dot(dl_s, heads[block * own + s], ((1,), (1,))).astype(bf16)
                    dpre[at, :] = (dfeat.astype(f32) * slopes[at, :]).astype(bf16)
            for p in range(n_hyper):
                block = (q - base) * n_hyper + p
                both = dpre[pl.ds(pl.multiple_of(block * tall, tall), tall), :]
                gw = gw + dot(xg[q, p, :tall, :], both, ((0,), (0,)))
                gb = gb + jnp.sum(both.astype(f32), axis=0, keepdims=True)
            gw_acc[...], gb_acc[...] = gw, gb
            return carry

        lax.fori_loop(0, 2, step, 0)

    def go_part(low, high):
        def step(g, carry):
            at = pl.ds(pl.multiple_of(g * DG, DG), DG)
            go[:, at, :] = dot(diag_t[...], dheads[g]).astype(bf16).reshape(hh, DG, classes)
            return carry

        if single:
            lax.fori_loop(low, high, step, 0)

    def total_part(q0):
        count = 2 * group * DG
        at = pl.ds(pl.multiple_of(q0 * group * DG, group * DG), count)
        z = dot(ho_group(0), dheads[0, at, :], ((1,), (1,)))
        for g in range(1, groups):
            z = z + dot(ho_group(g), dheads[g, at, :], ((1,), (1,)))
        d = lax.broadcasted_iota(i32, z.shape, 0) % DG
        same = d == lax.broadcasted_iota(i32, z.shape, 1) % DG
        kept = jnp.sum(jnp.where(same, z, 0.0).reshape(hh, DG, count), axis=1)
        kept = jnp.concatenate([kept, jnp.zeros((128 - hh, count), f32)], axis=0)
        fold = lax.broadcasted_iota(i32, (2 * group, count), 1) // DG
        fold = (fold == lax.broadcasted_iota(i32, (2 * group, count), 0)).astype(f32)
        mine = dot(fold, kept, ((1,), (1,)), precision=highest)
        dh_mine[pl.ds(pl.multiple_of(q0 * group, group), 2 * group), :] = mine

    def flood_first(flood, work, count):
        cuts = [count * (t + 1) // na for t in range(na)]
        done = 0
        for t in range(1, na):
            work(done, cuts[t - 1])
            done = cuts[t - 1]
            flood.column(t)
            flood.pair(t - 1)
            flood.across(t - 1)
        flood.corner(0)
        work(done, count)
        flood.pair(na - 1)
        flood.across(na - 1)

    get_h.wait()
    if single:
        flood_first(grads, heads_part, groups)
        for t in range(na):
            if t + 1 < na:
                grads.corner(t + 1)
            grads.near(t)
            grads.far(t)
            slots_part(0, source(grads.a, t, na) * 2)
            if t + 1 < na:
                total_part(source(grads.a, t, na) * 2)
    else:
        flood_first(grads, lambda low, high: None, groups)
        for t in range(na):
            if t + 1 < na:
                grads.corner(t + 1)
            grads.near(t)
            grads.far(t)

        def one(q, carry):
            prepare(q * nq)
            heads_part(0, groups)
            for n in range(nq // 2):
                slots_part(q * nq, q * nq + 2 * n)
            for n in range(nq // 2):
                total_part(q * nq + 2 * n)
            diag_t[...] = spread_t(hid_out[pl.ds(pl.multiple_of(q * CS, CS), CS), :])
            at = pl.ds(pl.multiple_of(q * CS * DG, CS * DG), CS * DG)
            for g in range(groups):
                spot = slice(g * DG, (g + 1) * DG)
                go_acc[:, spot, :] += dot(diag_t[...], dheads[g, at, :]).reshape(hh, DG, classes)
            return carry

        go_acc[...] = jnp.zeros_like(go_acc)

        lax.fori_loop(0, n_dp // nq, one, 0)
        go[...] = go_acc[...].astype(bf16)
    gw_own[:width] = gw_acc[...].astype(bf16)
    gw_own[width:] = jnp.broadcast_to(gb_acc[...], (16, narrow)).astype(bf16)
    if aligned:
        gw_all[i, j] = gw_own[...]
    else:
        put_own = pltpu.make_async_copy(gw_own, gw_all.at[i, j], local_sems.at[2])
        put_own.start()
        put_own.wait()
    fin = Flood(gw_all, floods[2 * count :], n_dp, half)
    fin.begin(gw_own)
    if single:
        total_part(source(grads.a, na - 1, na) * 2)

    share = slots // n_hyper
    peers = [lax.rem(j + u, n_hyper) for u in range(1, n_hyper)]
    to_hyper = []
    for u in range(1, n_hyper):
        at = pl.ds(pl.multiple_of(peers[u - 1] * share, share), share)
        copy = remote(dh_mine.at[at], b1.at[u], sa.at[u], ra.at[u], i, peers[u - 1])
        copy.start()
        to_hyper.append(copy)
    quart = groups // 4
    go_part(0, quart)
    fin.column(1)
    fin.pair(0)
    fin.across(0)
    quarter = dh_mine[pl.ds(pl.multiple_of(j * share, share), share), :]
    for u in range(1, n_hyper):
        to_hyper[u - 1].wait_recv()
        quarter = quarter + b1[u]
    dh_sum[0] = quarter
    b2[i] = quarter
    to_dp = []
    for t in range(1, n_dp):
        copy = remote(dh_sum.at[0], b2.at[i], sb.at[t], rb.at[t], swap(i, t, n_dp), j)
        copy.start()
        to_dp.append(copy)
    go_part(quart, 2 * quart)
    for t in range(2, na):
        fin.column(t)
        fin.pair(t - 1)
        fin.across(t - 1)
    fin.corner(0)
    go_part(2 * quart, 3 * quart)
    for copy in to_dp:
        copy.wait_recv()
    sum_all = b2[0]
    for t in range(1, n_dp):
        sum_all = sum_all + b2[t]
    dh_sum[1] = sum_all
    dh_all[j] = sum_all
    last = []
    for u in range(1, n_hyper):
        copy = remote(dh_sum.at[1], dh_all.at[j], sc.at[u], rc.at[u], i, peers[u - 1])
        copy.start()
        last.append(copy)
    fin.pair(na - 1)
    fin.across(na - 1)
    go_part(3 * quart, groups)
    put_go = pltpu.make_async_copy(go, go_out, local_sems.at[3])
    put_go.start()
    for t in range(1, na):
        fin.corner(t)
    for t in range(na):
        fin.near(t)
        fin.far(t)
    for copy in last:
        copy.wait_recv()
    put_go.wait()
    for copy in list(to_partner.values()) + list(to_peer.values()) + to_hyper + to_dp + last + to_ids:
        copy.wait_send()
    for flood in (inp, grads, fin):
        flood.end()


def main_part(x, ids, labels, ew, eb, wn, bn, emb, hin_t, hb, ho, n_dp, n_hyper, aligned):
    own, rows = labels.shape
    tall, width = x.shape
    hh, wide, classes = ho.shape
    narrow = wide // n_dp
    half = n_hyper // 2
    group = n_hyper * own
    slots = group * n_dp
    CS = slots if slots <= 64 else 2 * group
    chunk = 128
    depth = 3 if slots <= 64 else 2
    block = tall + 16
    share = slots // n_hyper
    dma = pltpu.SemaphoreType.DMA
    sample = CS * rows
    vm = pltpu.VMEM
    ANY = pl.BlockSpec(memory_space=pl.ANY)
    shape = jax.ShapeDtypeStruct
    return pl.pallas_call(
        functools.partial(main_kernel, n_dp, half, own, rows, aligned),
        out_shape=(
            shape((n_dp, n_hyper, width + 16, narrow), bf16),
            shape((n_hyper, share, 128), f32),
            shape((hh, narrow, classes), bf16),
            shape((slots, hh), f32),
            shape((slots, emb.shape[1]), bf16),
            shape((slots, emb.shape[0]), bf16),
        ),
        in_specs=[VM, pl.BlockSpec(memory_space=pltpu.SMEM), VM, ANY, VM, VM, VM, VM, VM, VM, ANY],
        out_specs=(VM if aligned else ANY, VM, ANY, VM, VM, VM),
        scratch_shapes=[
            vm((block, width), bf16),
            vm((n_dp, n_hyper, block, width), bf16),
            vm((n_dp, n_hyper, tall, classes), bf16),
            vm((tall, classes), bf16),
            vm((width, wide), bf16),
            vm((width, narrow), bf16),
            vm((depth, hh, chunk, classes), bf16),
            vm((hh, narrow, classes), bf16),
            vm((group * HG, hh * HG), bf16),
            vm((group, chunk, classes), bf16),
            vm((n_hyper, tall, classes), f32),
            vm((half, tall, classes), f32),
            vm((half, tall, classes), f32),
            vm((half, tall, classes), f32),
            vm((CS * HG, hh * HG), bf16),
            vm((CS, narrow, classes), bf16),
            vm((narrow // DG, slots * DG, classes), bf16),
            vm((hh * DG, CS * DG), bf16),
            vm((hh, narrow, classes), bf16),
            vm((8, 8, 128) if CS == slots else (hh, narrow, classes), f32),
            vm((sample, narrow), bf16),
            vm((sample, narrow), f32),
            vm((sample, narrow), bf16),
            vm((width, narrow), f32),
            vm((1, narrow), f32),
            vm((width + 16, narrow), bf16),
            vm((slots, 128), f32),
            vm((n_hyper, share, 128), f32),
            vm((n_dp, share, 128), f32),
            vm((2, share, 128), f32),
            vm((slots, hh), bf16),
            vm((1, wide), f32),
            vm((16, width), bf16),
            vm((n_hyper, 16, width), bf16),
            dma((4,)),
            dma((depth,)),
        ]
        + [dma((half,)) for _ in range(4)]
        + [dma((n_hyper,)), dma((n_hyper,))]
        + [dma((n_hyper,)), dma((n_hyper,)), dma((n_dp,)), dma((n_dp,)), dma((n_hyper,)), dma((n_hyper,))]
        + Flood.scratch(n_dp, half) * 3,
        compiler_params=pltpu.CompilerParams(
            collective_id=0, has_side_effects=True, vmem_limit_bytes=LIMIT
        ),
        name="main_part",
    )(x, ids, labels, ew, eb, wn, bn, emb, hin_t, hb, ho)


def last_kernel(aligned, pieces, go_in, gw_in, pre_ref, picked_ref, select_ref, hin_ref, dh_ref,
                go_out, gwf_out, gb_ref, table_ref, in_ref, hb_ref, go_b, go_f, gw_ref, gwf_ref, sems):
    hh, wide, _ = go_b.shape
    per = wide // pieces
    reads, writes = [], []
    for n in range(pieces):
        at = slice(n * per, (n + 1) * per)
        reads.append(pltpu.make_async_copy(go_in.at[:, at, :], go_b.at[:, at, :], sems.at[0, n]))
        writes.append(pltpu.make_async_copy(go_f.at[:, at, :], go_out.at[:, at, :], sems.at[1, n]))
        reads[n].start()
    get = pltpu.make_async_copy(gw_in, gw_ref, sems.at[2, 0])
    put = pltpu.make_async_copy(gwf_ref, gwf_out, sems.at[2, 1])
    if aligned:
        get.start()
    for n in range(pieces):
        at = slice(n * per, (n + 1) * per)
        reads[n].wait()
        go_f[:, at, :] = go_b[:, at, :].astype(f32)
        writes[n].start()
    if aligned:
        get.wait()
        n_dp, n_hyper, tall, narrow = gw_ref.shape
        for jj in range(n_hyper):
            for ii in range(n_dp):
                at = (jj * n_dp + ii) * narrow
                gwf_ref[:, at : at + narrow] = gw_ref[ii, jj, : tall - 16, :].astype(f32)
                gb_ref[:, at : at + narrow] = gw_ref[ii, jj, tall - 16 : tall - 8, :].astype(f32)[:1]
        put.start()
    dpre = dh_ref[...][:, :hh] * silu_slope(pre_ref[...])
    hb_ref[...] = jnp.sum(dpre, axis=0, keepdims=True)
    in_ref[...] = dot(dpre, picked_ref[...].astype(f32), ((0,), (0,)), precision=highest)
    back = dot(dpre, hin_ref[...].astype(f32), precision=highest)
    table_ref[...] = dot(select_ref[...].astype(f32), back, ((0,), (0,)), precision=highest)
    for copy in writes:
        copy.wait()
    if aligned:
        put.wait()


def last_part(go, pre, picked, select, hin_t, dh, gw_all, aligned):
    hh, wide, classes = go.shape
    width = picked.shape[1]
    clients = select.shape[1]
    n_dp, n_hyper, block, narrow = gw_all.shape
    shape = jax.ShapeDtypeStruct
    full = (block - 16, n_dp * n_hyper * narrow) if aligned else (8, 128)
    given = gw_all if aligned else gw_all[:1, :1]
    pieces = 4 if wide % 64 == 0 else 1
    ANY = pl.BlockSpec(memory_space=pl.ANY)
    return pl.pallas_call(
        functools.partial(last_kernel, aligned, pieces),
        out_shape=(
            shape(go.shape, f32),
            shape(full, f32),
            shape((1, full[1]), f32),
            shape((clients, hin_t.shape[1]), f32),
            shape((hh, width), f32),
            shape((1, hh), f32),
        ),
        in_specs=[ANY, ANY, VM, VM, VM, VM, VM],
        out_specs=(ANY, ANY, VM, VM, VM, VM),
        scratch_shapes=[
            pltpu.VMEM(go.shape, bf16),
            pltpu.VMEM(go.shape, f32),
            pltpu.VMEM(given.shape, bf16),
            pltpu.VMEM(full, f32),
            pltpu.SemaphoreType.DMA((3, 4)),
        ],
        compiler_params=pltpu.CompilerParams(vmem_limit_bytes=LIMIT),
        name="last_part",
    )(go, given, pre, picked, select, hin_t, dh)


def local(
    inputs, labels, client_ids, ext_weight, ext_bias, embeddings, hyper_in, hyper_bias, hyper_out
):
    n_dp, n_hyper = lax.axis_size("dp"), lax.axis_size("hyper")
    own, rows, width = inputs.shape
    narrow = hyper_out.shape[0] // n_dp
    aligned = narrow % 128 == 0
    ho = hyper_out.transpose(1, 0, 2)
    hin_t = hyper_in.T
    bias = ext_bias
    if aligned:
        wn, bn = embeddings, hyper_bias[None]
    else:
        start = (lax.axis_index("hyper") * n_dp + lax.axis_index("dp")) * narrow
        wn = lax.dynamic_slice_in_dim(ext_weight, start, narrow, 1)
        bn = lax.dynamic_slice_in_dim(bias, start, narrow, 0)[None]
    gw_all, dh, go, pre, picked, select = main_part(
        inputs.reshape(own * rows, width), client_ids, labels, ext_weight, bias, wn, bn,
        embeddings, hin_t, hyper_bias[None], ho, n_dp, n_hyper, aligned,
    )
    grad_out, gw, gb, table, grad_in, grad_hb = last_part(
        go, pre, picked, select, hin_t, dh.reshape(-1, 128), gw_all, aligned
    )
    if not aligned:
        gw = gw_all[:, :, :width].transpose(2, 1, 0, 3).reshape(width, -1).astype(f32)
        gb = gw_all[:, :, width].transpose(1, 0, 2).reshape(-1).astype(f32)
    return (gw, gb.reshape(-1), table, grad_in.T, grad_hb.reshape(-1), grad_out.transpose(1, 0, 2))


def solution(mesh):
    placed = (
        P(("dp", "hyper"), None, None),
        P(("dp", "hyper"), None),
        P(("dp", "hyper")),
        P(),
        P(),
        P(),
        P(),
        P(),
        P("hyper", None, None),
    )
    return jax.shard_map(
        local,
        mesh=mesh,
        in_specs=placed,
        out_specs=(P(), P(), P(), P(), P(), P(("hyper", "dp"), None, None)),
        check_vma=False,
    )
```
